32 devices in a mesh: rep: 4 (over x, y), dp: 8 (over z, core).
Axes of the slice: x: 2, y: 2, z: 4, core: 2. Of those that a mesh axis runs over, the one named last changes fastest.
Arguments:
- x: bfloat16 [32, 2048, 768], P(('rep', 'dp')), parts along dimension 0
- dy: bfloat16 [32, 2048, 768], P(('rep', 'dp')), parts along dimension 0
- w_gate: bfloat16 [2, 768, 1792], replicated
- w_up: bfloat16 [2, 768, 1792], replicated
- w_down: bfloat16 [2, 1792, 768], replicated
- m_w_gate: float32 [2, 768, 1792], replicated
- m_w_up: float32 [2, 768, 1792], replicated
- m_w_down: float32 [2, 1792, 768], replicated
- v_w_gate: float32 [2, 768, 1792], replicated
- v_w_up: float32 [2, 768, 1792], replicated
- v_w_down: float32 [2, 1792, 768], replicated
Outputs:
- output 1: bfloat16 [8, 768, 1792], P('rep'), parts along dimension 0
- output 2: bfloat16 [8, 768, 1792], P('rep'), parts along dimension 0
- output 3: bfloat16 [8, 1792, 768], P('rep'), parts along dimension 0
- output 4: float32 [8, 768, 1792], P('rep'), parts along dimension 0
- output 5: float32 [8, 768, 1792], P('rep'), parts along dimension 0
- output 6: float32 [8, 1792, 768], P('rep'), parts along dimension 0
- output 7: float32 [8, 768, 1792], P('rep'), parts along dimension 0
- output 8: float32 [8, 768, 1792], P('rep'), parts along dimension 0
- output 9: float32 [8, 1792, 768], P('rep'), parts along dimension 0
There are 4 independent parts. The reference program is written for one: setup_inputs(seed, part) draws one part's arguments, and reference() takes and returns one part's arrays. A program takes and returns all parts, laid end to end along the dimension named above; an argument that names none is the same for every part.
All inputs are finite; a program needn't handle non-finite values.
Results may differ from the reference program's by a relative error of at most 0.022.
Values are sent between devices in bfloat16 or wider.
A program may use at most 2.25 GiB of HBM per device.

```python
import jax
import jax.numpy as jnp
from jax import lax

SEQUENCES = 8
TOKENS = 2048
D = 768
FF = 1792
LAYERS = 2
NAMES = ("w_gate", "w_up", "w_down")
SHAPES = {"w_gate": (LAYERS, D, FF), "w_up": (LAYERS, D, FF), "w_down": (LAYERS, FF, D)}


def bump(key, n, height):
    away = (jnp.arange(n, dtype=jnp.int32) - jax.random.randint(key, (), 0, n, jnp.int32)) % n
    return jnp.where(away < n // 8, height, 1.0)


def together(key, own, strength):
    shared = jax.random.normal(key, own.shape[1:], jnp.float32)
    return (own + strength * shared) * lax.rsqrt(1 + strength * strength)


def setup_inputs(seed: int = 0, part: int = 0) -> dict:
    kx, kdy, ka, kb, kz, kf, kh, kl, *keys = jax.random.split(jax.random.key(seed), 8 + 3 * len(NAMES))
    kx, kdy, ka, kb = (jax.random.fold_in(k, part) for k in (kx, kdy, ka, kb))
    kw, km, kv = (keys[i::3] for i in range(3))
    shape = (SEQUENCES, TOKENS, D)
    much_x, much_dy = jax.random.uniform(kz, (2,), jnp.float32, 0.0, 1.0)
    loud = 2.0 ** jax.random.uniform(jax.random.fold_in(kz, 1), (), jnp.float32, -1.0, 2.0)
    layers = 2.0 ** jax.random.uniform(kl, (LAYERS, 1, 1), jnp.float32, -1.0, 1.0)
    x = together(ka, jax.random.normal(kx, shape, jnp.float32), much_x) * bump(kf, D, 4.0)
    dy = together(kb, jax.random.normal(kdy, shape, jnp.float32), much_dy)
    drawn = {"x": x.astype(jnp.bfloat16), "dy": (loud * dy * (SEQUENCES * TOKENS) ** -0.5).astype(jnp.bfloat16)}
    for key, name in zip(kw, NAMES, strict=True):
        w = jax.random.normal(key, SHAPES[name], jnp.float32) * SHAPES[name][1] ** -0.5
        drawn[name] = (w * {"w_gate": 1.0, "w_up": bump(kh, FF, 4.0), "w_down": layers}[name]).astype(jnp.bfloat16)
    for key, name in zip(km, NAMES, strict=True):
        drawn[f"m_{name}"] = 0.1 * jax.random.normal(key, SHAPES[name], jnp.float32)
    for key, name in zip(kv, NAMES, strict=True):
        drawn[f"v_{name}"] = jax.random.uniform(key, SHAPES[name], jnp.float32, 0.005, 0.015)
    return drawn


def matmul(a, w):
    return jnp.dot(a, w, preferred_element_type=jnp.float32).astype(jnp.bfloat16)


def normed(h):
    wide = h.astype(jnp.float32)
    scale = lax.rsqrt(jnp.mean(wide**2, -1, keepdims=True) + 1e-6)
    return (wide * scale).astype(jnp.bfloat16)


def layer(h, w):
    a = normed(h)
    gate = jnp.dot(a, w["w_gate"], preferred_element_type=jnp.float32)
    up = jnp.dot(a, w["w_up"], preferred_element_type=jnp.float32)
    return h + matmul((jax.nn.silu(gate) * up).astype(jnp.bfloat16), w["w_down"])


def adamw(w, m, v, g):
    m = 0.9 * m + 0.1 * g
    v = 0.95 * v + 0.05 * g * g
    step = m * lax.rsqrt(v + 1e-8) + 0.1 * w
    return (w - 0.02 * step).astype(jnp.bfloat16), m, v


def clipped(gradients, sum_of_squares, count):
    factor = jnp.minimum(1.0, 0.5 * lax.rsqrt(sum_of_squares / count + 1e-30))
    return [g * factor for g in gradients]


def stack(weights, h):
    return lax.scan(lambda h, w: (layer(h, w), None), h, weights)[0]


def reference(x, dy, w_gate, w_up, w_down, m_w_gate, m_w_up, m_w_down, v_w_gate, v_w_up, v_w_down):
    weights = dict(zip(NAMES, (w_gate, w_up, w_down), strict=True))

    def take(so_far, sequence):
        h, by_y = sequence
        _, back = jax.vjp(lambda w: stack(w, h), weights)
        return jax.tree.map(lambda total, term: total + term.astype(jnp.float32), so_far, back(by_y)[0]), None

    none_yet = {name: jnp.zeros(w.shape, jnp.float32) for name, w in weights.items()}
    by_weights, _ = lax.scan(take, none_yet, (x, dy))
    gradients = [by_weights[name].astype(jnp.bfloat16).astype(jnp.float32) for name in NAMES]
    gradients = clipped(gradients, sum(jnp.sum(g * g) for g in gradients), sum(g.size for g in gradients))
    new = [
        adamw(w.astype(jnp.float32), m, v, g)
        for w, m, v, g in zip((w_gate, w_up, w_down), (m_w_gate, m_w_up, m_w_down), (v_w_gate, v_w_up, v_w_down), gradients, strict=True)
    ]
    return tuple(one[which] for which in range(3) for one in new)
```

```python
import jax
import jax.numpy as jnp
from jax import lax
from jax.experimental import pallas as pl
from jax.experimental.pallas import tpu as pltpu
from jax.sharding import PartitionSpec as P

NAMES = ("w_gate", "w_up", "w_down")


def matmul(a, w):
    return jnp.dot(a, w, preferred_element_type=jnp.float32).astype(jnp.bfloat16)


def normed(h):
    wide = h.astype(jnp.float32)
    scale = lax.rsqrt(jnp.mean(wide**2, -1, keepdims=True) + 1e-6)
    return (wide * scale).astype(jnp.bfloat16)


def layer(h, w):
    a = normed(h)
    gate = jnp.dot(a, w["w_gate"], preferred_element_type=jnp.float32)
    up = jnp.dot(a, w["w_up"], preferred_element_type=jnp.float32)
    return h + matmul((jax.nn.silu(gate) * up).astype(jnp.bfloat16), w["w_down"])


def adamw(w, m, v, g):
    m = 0.9 * m + 0.1 * g
    v = 0.95 * v + 0.05 * g * g
    step = m * lax.rsqrt(v + 1e-8) + 0.1 * w
    return (w - 0.02 * step).astype(jnp.bfloat16), m, v


def clipped(gradients, sum_of_squares, count):
    factor = jnp.minimum(1.0, 0.5 * lax.rsqrt(sum_of_squares / count + 1e-30))
    return [g * factor for g in gradients]


MESH = pl.DeviceIdType.MESH
MATS = 6
ROWS, COLS = 768, 1792
HALF, QUARTER = ROWS // 2, ROWS // 4
SUB = 4
PIECE = QUARTER // SUB
N = MATS * SUB
SKEW = 2
LINE = 4


def place(q):
    return lax.rem(lax.rem(q, 3) + 2, 3) * 2 + 1 - q // 3


def sum_kernel(*refs):
    terms = refs[:MATS]
    out, squares_out, t, p, r, acc, tile, sq, load, xs, xr, right_s, left_s, rs_r, ag_r, d_s, d_r, out_s, sq_s, sq_r = refs[MATS:]
    dp = lax.axis_index("dp")
    z, c = dp // 2, lax.rem(dp, 2)
    other = z * 2 + 1 - c

    loads = [pltpu.make_async_copy(terms[m], t.at[pl.ds(m * ROWS, ROWS)], load.at[m]) for m in range(MATS)]
    order = [4 + 1, 0 + 1, 2 + 1, 4, 0, 2]
    for m in order:
        loads[m].start()
    barrier = pltpu.get_barrier_semaphore()
    for step in range(1, 8):
        pl.semaphore_signal(barrier, inc=1, device_id={"dp": lax.rem(dp + step, 8)}, device_id_type=MESH)
    pl.semaphore_wait(barrier, 7)
    acc[...] = jnp.zeros_like(acc)

    def exchange(m, x):
        return pltpu.make_async_remote_copy(
            src_ref=t.at[pl.ds(pl.multiple_of(m * ROWS + (1 - c) * HALF + x * QUARTER, 16), QUARTER)],
            dst_ref=p.at[pl.ds(pl.multiple_of(m * HALF + x * QUARTER, 16), QUARTER)],
            send_sem=xs,
            recv_sem=xr.at[x * MATS + m],
            device_id={"dp": other},
            device_id_type=MESH,
        )

    for m in order:
        loads[m].wait()
        for x in range(2):
            exchange(m, x).start()

    def wide(k, x, core):
        m = place(k // SUB)
        return pl.ds(pl.multiple_of(m * ROWS + core * HALF + x * QUARTER + lax.rem(k, SUB) * PIECE, 16), PIECE)

    def narrow(k, x):
        m = place(k // SUB)
        return pl.ds(pl.multiple_of(m * HALF + x * QUARTER + lax.rem(k, SUB) * PIECE, 16), PIECE)

    def sum_copy(k, x):
        return pltpu.make_async_remote_copy(
            src_ref=p.at[narrow(k, x)],
            dst_ref=r.at[narrow(k, x)],
            send_sem=right_s if x == 0 else left_s,
            recv_sem=rs_r.at[x * N + k],
            device_id={"dp": dp + 2 if x == 0 else dp - 2},
            device_id_type=MESH,
        )

    def back_copy(k, x, first=False):
        return pltpu.make_async_remote_copy(
            src_ref=r.at[narrow(k, x)] if first else out.at[wide(k, x, c)],
            dst_ref=out.at[wide(k, x, c)],
            send_sem=left_s if x == 0 else right_s,
            recv_sem=ag_r.at[x * N + k],
            device_id={"dp": dp - 2 if x == 0 else dp + 2},
            device_id_type=MESH,
        )

    def share_copy(k, x, first=False):
        return pltpu.make_async_remote_copy(
            src_ref=r.at[narrow(k, x)] if first else out.at[wide(k, x, c)],
            dst_ref=out.at[wide(k, x, c)],
            send_sem=d_s,
            recv_sem=d_r.at[x * N + k],
            device_id={"dp": other},
            device_id_type=MESH,
        )

    def share_arrival(k, x):
        return pltpu.make_async_remote_copy(
            src_ref=out.at[wide(k, x, 1 - c)],
            dst_ref=out.at[wide(k, x, 1 - c)],
            send_sem=d_s,
            recv_sem=d_r.at[x * N + k],
            device_id={"dp": other},
            device_id_type=MESH,
        )

    def valid(k):
        return jnp.logical_and(k >= 0, k < N)

    def add(k, x):
        hops = z if x == 0 else LINE - 1 - z

        @pl.when(lax.rem(k, SUB) == 0)
        def _():
            exchange(place(k // SUB), x).wait_recv()

        mine = t[wide(k, x, c), :].astype(jnp.float32) + p[narrow(k, x), :].astype(jnp.float32)

        @pl.when(hops == 0)
        def _():
            p[narrow(k, x), :] = mine.astype(jnp.bfloat16)
            sum_copy(k, x).start()

        @pl.when(hops > 0)
        def _():
            sum_copy(k, x).wait_recv()
            mine = t[wide(k, x, c), :].astype(jnp.float32) + p[narrow(k, x), :].astype(jnp.float32)
            total = (mine + r[narrow(k, x), :].astype(jnp.float32)).astype(jnp.bfloat16)

            @pl.when(hops < LINE - 1)
            def _():
                p[narrow(k, x), :] = total
                sum_copy(k, x).start()

            @pl.when(hops == LINE - 1)
            def _():
                r[narrow(k, x), :] = total
                back_copy(k, x, True).start()
                share_copy(k, x, True).start()
                pltpu.make_async_copy(r.at[narrow(k, x)], out.at[wide(k, x, c)], out_s).start()
                g = total.astype(jnp.float32)
                acc[...] += jnp.sum((g * g).reshape(PIECE // 8, 8, COLS), axis=0)

    def relay(k, x):
        back_copy(k, x).wait_recv()

        @pl.when((z if x == 0 else LINE - 1 - z) > 0)
        def _():
            back_copy(k, x).start()

        share_copy(k, x).start()

    turn = SKEW * (LINE - 1)

    @pl.loop(0, N + 2 * turn + 1)
    def _(i):
        for x in range(2):
            k = i - SKEW * (z if x == 0 else LINE - 1 - z)
            pl.when(valid(k))(lambda k=k, x=x: add(k, x))
        for x in range(2):
            back = LINE - 1 - z if x == 0 else z
            k = i - turn - SKEW * back
            pl.when(jnp.logical_and(back > 0, valid(k)))(lambda k=k, x=x: relay(k, x))
            k = k - 1

            @pl.when(valid(k))
            def _(k=k, x=x):
                share_arrival(k, x).wait_recv()

    total = jnp.sum(acc[...])
    tile[...] = jnp.full(tile.shape, total, jnp.float32)

    def tell(slot, step):
        return pltpu.make_async_remote_copy(
            src_ref=tile, dst_ref=sq.at[slot], send_sem=sq_s.at[step - 1], recv_sem=sq_r.at[slot],
            device_id={"dp": lax.rem(dp + step, 8)}, device_id_type=MESH,
        )

    for slot, owner in enumerate((0, 1, 6, 7)):
        @pl.when(dp == owner)
        def _(slot=slot):
            for step in range(1, 8):
                tell(slot, step).start()
            sq[slot] = tile[...]

        @pl.when(dp != owner)
        def _(slot=slot):
            tell(slot, 1).wait_recv()

    squares_out[...] = sq[0] + sq[1] + sq[2] + sq[3]

    for slot, owner in enumerate((0, 1, 6, 7)):
        @pl.when(dp == owner)
        def _(slot=slot):
            for step in range(1, 8):
                tell(slot, step).wait_send()

    def all_sent(sem):
        pltpu.make_async_remote_copy(
            src_ref=p, dst_ref=p, send_sem=sem, recv_sem=xr.at[0], device_id={"dp": other}, device_id_type=MESH
        ).wait_send()

    pl.when(z < LINE - 1)(lambda: all_sent(right_s))
    pl.when(z > 0)(lambda: all_sent(left_s))
    all_sent(d_s)
    all_sent(xs)

    @pl.when(jnp.logical_or(z == 0, z == LINE - 1))
    def _():
        pltpu.make_async_copy(r.at[pl.ds(0, N * PIECE)], out.at[pl.ds(0, N * PIECE)], out_s).wait()


def group_sum(terms):
    dma = pltpu.SemaphoreType.DMA
    vmem = pltpu.VMEM
    return pl.pallas_call(
        sum_kernel,
        out_shape=(jax.ShapeDtypeStruct((MATS * ROWS, COLS), jnp.bfloat16), jax.ShapeDtypeStruct((8, 128), jnp.float32)),
        in_specs=[pl.BlockSpec(memory_space=pl.ANY)] * MATS,
        out_specs=(pl.BlockSpec(memory_space=pl.ANY), pl.BlockSpec(memory_space=pltpu.VMEM)),
        scratch_shapes=[
            vmem((MATS * ROWS, COLS), jnp.bfloat16),
            vmem((MATS * HALF, COLS), jnp.bfloat16),
            vmem((MATS * HALF, COLS), jnp.bfloat16),
            vmem((8, COLS), jnp.float32),
            vmem((8, 128), jnp.float32),
            vmem((4, 8, 128), jnp.float32),
            dma((MATS,)), dma(()), dma((2 * MATS,)), dma(()), dma(()), dma((2 * N,)), dma((2 * N,)), dma(()), dma((2 * N,)), dma(()),
            dma((7,)), dma((4,)),
        ],
        compiler_params=pltpu.CompilerParams(collective_id=0, has_side_effects=True, vmem_limit_bytes=60 * 2**20),
        name="group_sum",
    )(*terms)


def solution(mesh):
    def step(x, dy, *arrays):
        weights, m, v = (arrays[i : i + 3] for i in (0, 3, 6))
        layers = weights[0].shape[0]
        h, kept = x[0], []
        for number in range(layers):
            kept.append(h)
            h = layer(h, {name: w[number] for name, w in zip(NAMES, weights, strict=True)})
        by_h, terms = dy[0], [None] * MATS
        for number in reversed(range(layers)):
            _, back = jax.vjp(lambda w, h: layer(h, w), {name: w[number] for name, w in zip(NAMES, weights, strict=True)}, kept[number])
            by_w, by_h = back(by_h)
            terms[number], terms[2 + number], terms[4 + number] = by_w["w_gate"], by_w["w_up"], by_w["w_down"].T
        summed, squares = group_sum(terms)
        summed = summed.reshape(3, layers, ROWS, COLS)
        gradients = [summed[0].astype(jnp.float32), summed[1].astype(jnp.float32), summed[2].transpose(0, 2, 1).astype(jnp.float32)]
        gradients = clipped(gradients, squares[0, 0], sum(g.size for g in gradients))
        new = [adamw(w.astype(jnp.float32), m, v, g) for w, m, v, g in zip(weights, m, v, gradients, strict=True)]
        return tuple(one[which] for which in range(3) for one in new)

    return jax.shard_map(
        step,
        mesh=mesh,
        in_specs=(P(("rep", "dp"), None, None),) * 2 + (P(None, None, None),) * 9,
        out_specs=(P("rep", None, None),) * 9,
        check_vma=False,
    )
```

```python
import functools

import jax
import jax.numpy as jnp
from jax import lax
from jax.experimental import pallas as pl
from jax.experimental.pallas import tpu as pltpu
from jax.sharding import PartitionSpec as P

BF, F32 = jnp.bfloat16, jnp.float32


def dot(a, b):
    return jnp.dot(a, b, preferred_element_type=F32)


def dot_t(a, b):
    return lax.dot_general(a, b, (((1,), (1,)), ((), ())), preferred_element_type=F32)


def normed(h):
    wide = h.astype(F32)
    scale = lax.rsqrt(jnp.mean(wide**2, -1, keepdims=True) + 1e-6)
    return (wide * scale).astype(BF)


def sigmoid(x):
    return 1.0 / (1.0 + jnp.exp(-x))


def by_gate_and_up(gate, up, by_p):
    s = sigmoid(gate)
    silu = gate * s
    by_p = by_p.astype(BF).astype(F32)
    return (by_p * up * (s + silu * (1.0 - s))).astype(BF), (by_p * silu).astype(BF), (silu * up).astype(BF)


TOKENS, ROWS, COLS = 2048, 768, 1792
BLOCK = 512
TILE = 256
TILES = COLS // TILE


def forward_kernel(x, dy, w_gate, w_up, w_down, a0_out, p0_out, h1_out, a1_out, p1_out, bg_out, bu_out, *scratch):
    weights, sem = scratch[:6], scratch[6]
    copies = [pltpu.make_async_copy(w.at[n], weights[3 * n + i], sem.at[3 * n + i]) for n in range(2) for i, w in enumerate((w_gate, w_up, w_down))]

    first = pl.program_id(0) == 0

    @pl.when(first)
    def _():
        for copy in copies:
            copy.start()

    a0 = normed(x[...])
    a0_out[...] = a0

    def ready(*which):
        @pl.when(first)
        def _():
            for i in which:
                copies[i].wait()

    ready(0, 1)
    for n in range(TILES):
        at = slice(n * TILE, (n + 1) * TILE)
        gate, up = dot(a0_out[...], weights[0][:, at]), dot(a0_out[...], weights[1][:, at])
        p0_out[:, at] = (gate * sigmoid(gate) * up).astype(BF)
    ready(2)
    h1_out[...] = x[...] + dot(p0_out[...], weights[2][...]).astype(BF)
    a1_out[...] = normed(h1_out[...])
    ready(3, 4, 5)
    for n in range(TILES):
        at = slice(n * TILE, (n + 1) * TILE)
        gate, up = dot(a1_out[...], weights[3][:, at]), dot(a1_out[...], weights[4][:, at])
        bg_out[:, at], bu_out[:, at], p1_out[:, at] = by_gate_and_up(gate, up, dot_t(dy[...], weights[5][at, :]))


def forward(x, dy, w_gate, w_up, w_down):
    narrow, wide = pl.BlockSpec((BLOCK, ROWS), lambda i: (i, 0)), pl.BlockSpec((BLOCK, COLS), lambda i: (i, 0))
    of = lambda n: jax.ShapeDtypeStruct((TOKENS, n), BF)
    return pl.pallas_call(
        forward_kernel,
        grid=(TOKENS // BLOCK,),
        out_shape=(of(ROWS), of(COLS), of(ROWS), of(ROWS), of(COLS), of(COLS), of(COLS)),
        in_specs=[narrow, narrow] + [pl.BlockSpec(memory_space=pl.ANY)] * 3,
        out_specs=(narrow, wide, narrow, narrow, wide, wide, wide),
        scratch_shapes=[pltpu.VMEM(s, BF) for _ in range(2) for s in ((ROWS, COLS), (ROWS, COLS), (COLS, ROWS))] + [pltpu.SemaphoreType.DMA((6,))],
        compiler_params=pltpu.CompilerParams(vmem_limit_bytes=60 * 2**20),
        name="forward",
    )(x, dy, w_gate, w_up, w_down)


def adamw_kernel(transposed, squares, g, w, m, v, w_out, m_out, v_out):
    count = 2 * 3 * ROWS * COLS
    factor = jnp.minimum(1.0, 0.5 * lax.rsqrt(squares[...] / count + 1e-30))[0:1, 0:1]
    g = (g[...].T if transposed else g[...]).astype(F32) * factor
    m = 0.9 * m[0] + 0.1 * g
    v = 0.95 * v[0] + 0.05 * g * g
    w = w[0].astype(F32)
    w_out[0] = (w - 0.02 * (m * lax.rsqrt(v + 1e-8) + 0.1 * w)).astype(BF)
    m_out[0] = m
    v_out[0] = v


def adamw(kind, squares, summed, w, m, v):
    transposed = w.shape[1] == COLS
    layers = w.shape[0]
    block = 256
    if transposed:
        steps = COLS // block
        own, grad = pl.BlockSpec((1, block, ROWS), lambda n, i: (n, i, 0)), pl.BlockSpec((ROWS, block), lambda n, i: (kind * layers + n, i))
    else:
        steps = ROWS // block
        own, grad = pl.BlockSpec((1, block, COLS), lambda n, i: (n, i, 0)), pl.BlockSpec((block, COLS), lambda n, i: ((kind * layers + n) * steps + i, 0))
    return pl.pallas_call(
        functools.partial(adamw_kernel, transposed),
        grid=(layers, steps),
        out_shape=(jax.ShapeDtypeStruct(w.shape, BF), jax.ShapeDtypeStruct(w.shape, F32), jax.ShapeDtypeStruct(w.shape, F32)),
        in_specs=[pl.BlockSpec((8, 128), lambda n, i: (0, 0)), grad, own, own, own],
        out_specs=(own, own, own),
        compiler_params=pltpu.CompilerParams(vmem_limit_bytes=60 * 2**20),
        name="adamw",
    )(squares, summed, w, m, v)


MESH = pl.DeviceIdType.MESH
MATS = 6
HALF, QUARTER = ROWS // 2, ROWS // 4
SUB = 4
PIECE = QUARTER // SUB
N = MATS * SUB
SKEW = 2
LINE = 4


def place(q):
    return lax.rem(lax.rem(q, 3) + 2, 3) * 2 + 1 - q // 3


SLOTS = 4


def backward_kernel(*refs):
    dy_in, a0_in, p0_in, h1_in, a1_in, p1_in, bg_in, bu_in, wg_in, wu_in, wd_in = refs[:11]
    out, squares_out, t, p, r, bg, bu, lhs, by_h, small, wg, wu, wd, acc, tile, sq = refs[11:27]
    load, xs, xr, right_s, left_s, rs_r, ag_r, d_s, d_r, out_s, sq_s, sq_r = refs[27:]
    dp = lax.axis_index("dp")
    z, c = dp // 2, lax.rem(dp, 2)
    other = z * 2 + 1 - c

    def fetch(src, dst, n):
        return pltpu.make_async_copy(src, dst, load.at[n])

    get_dy, get_p1, get_bg = fetch(dy_in, by_h, 0), fetch(p1_in, bu, 1), fetch(bg_in, bg, 2)
    get_a1, get_wg1, get_wu1, get_wd0 = fetch(a1_in, small, 3), fetch(wg_in.at[1], wg, 4), fetch(wu_in.at[1], wu, 5), fetch(wd_in.at[0], wd, 6)
    get_bu, get_h1 = fetch(bu_in, bu, 7), fetch(h1_in, small, 8)
    get_p0, get_a0, get_wg0, get_wu0 = fetch(p0_in, bu, 9), fetch(a0_in, small, 10), fetch(wg_in.at[0], wg, 11), fetch(wu_in.at[0], wu, 12)
    for copy in (get_dy, get_p1, get_bg, get_a1, get_wg1, get_wu1, get_wd0):
        copy.start()
    barrier = pltpu.get_barrier_semaphore()
    for step in range(1, 8):
        pl.semaphore_signal(barrier, inc=1, device_id={"dp": lax.rem(dp + step, 8)}, device_id_type=MESH)
    pl.semaphore_wait(barrier, 7)
    acc[...] = jnp.zeros_like(acc)

    def own(q, row, rows):
        return pl.ds(pl.multiple_of(lax.rem(q, SLOTS) * ROWS + row, 16), rows)

    def exchange(q, x):
        return pltpu.make_async_remote_copy(
            src_ref=t.at[own(q, (1 - c) * HALF + x * QUARTER, QUARTER)],
            dst_ref=p.at[pl.ds(pl.multiple_of(place(q) * HALF + x * QUARTER, 16), QUARTER)],
            send_sem=xs.at[x * MATS + q],
            recv_sem=xr.at[x * MATS + q],
            device_id={"dp": other},
            device_id_type=MESH,
        )

    def turned(src):
        @pl.loop(0, TOKENS // TILE)
        def _(i):
            at = pl.ds(pl.multiple_of(i * TILE, TILE), TILE)
            lhs[:, at] = src[at, :].T

    def gradient(q, right, lo, hi):
        @pl.loop(lo, hi)
        def _(n):
            at = pl.ds(pl.multiple_of(n * TILE, TILE), TILE)
            t[own(q, 0, ROWS), at] = dot(lhs[...], right[:, at]).astype(BF)

    def send_terms(q):
        for x in range(2):
            exchange(q, x).start()

    get_dy.wait()
    turned(by_h)
    get_p1.wait()
    gradient(0, bu, 0, TILES)
    send_terms(0)
    get_bu.start()

    def through_layer(i):
        at = pl.ds(pl.multiple_of(i * BLOCK, BLOCK), BLOCK)
        by_a = dot_t(bg[at, :], wg[...]).astype(BF) + dot_t(bu[at, :], wu[...]).astype(BF)
        by_a, wide_h = by_a.astype(F32), small[at, :].astype(F32)
        scale = lax.rsqrt(jnp.mean(wide_h * wide_h, -1, keepdims=True) + 1e-6)
        inner = jnp.mean(by_a * wide_h, -1, keepdims=True)
        by_h[at, :] = by_h[at, :] + (by_a * scale - wide_h * (scale * scale * scale * inner)).astype(BF)

    def first_layer(i):
        rows = pl.ds(pl.multiple_of(i // TILES * BLOCK, BLOCK), BLOCK)
        at = pl.ds(pl.multiple_of(lax.rem(i, TILES) * TILE, TILE), TILE)
        gate, up = dot(small[rows, :], wg[:, at]), dot(small[rows, :], wu[:, at])
        bg[rows, at], bu[rows, at], _ = by_gate_and_up(gate, up, dot_t(by_h[rows, :], wd[at, :]))

    def work(i):
        @pl.when(i == 0)
        def _():
            get_a1.wait()
            turned(small)
            get_h1.start()
            get_bg.wait()

        @pl.when(i < 3)
        def _():
            gradient(1, bg, lax.select(i == 0, 0, 3 * i - 1), jnp.minimum(3 * i + 2, TILES))

        @pl.when(i == 2)
        def _():
            send_terms(1)

        @pl.when(i == 3)
        def _():
            get_bu.wait()

        @pl.when(jnp.logical_and(i >= 3, i < 6))
        def _():
            gradient(2, bu, 3 * (i - 3), jnp.minimum(3 * (i - 2), TILES))

        @pl.when(i == 5)
        def _():
            send_terms(2)

        @pl.when(i == 4)
        def _():
            for copy in (get_wg1, get_wu1, get_h1):
                copy.wait()

        @pl.when(jnp.logical_and(i >= 4, i < 8))
        def _():
            through_layer(i - 4)

        @pl.when(i == 7)
        def _():
            for copy in (get_p0, get_a0, get_wg0, get_wu0):
                copy.start()

        @pl.when(i == 8)
        def _():
            turned(by_h)
            get_p0.wait()

        @pl.when(jnp.logical_and(i >= 8, i < 11))
        def _():
            gradient(3, bu, lax.select(i == 8, 0, 3 * (i - 8) - 1), jnp.minimum(3 * (i - 8) + 2, TILES))

        @pl.when(i == 10)
        def _():
            send_terms(3)

        @pl.when(i == 11)
        def _():
            for copy in (get_a0, get_wg0, get_wu0, get_wd0):
                copy.wait()
            turned(small)

        @pl.when(jnp.logical_and(i >= 11, i < 15))
        def _():
            pl.loop(0, TILES)(lambda n: first_layer((i - 11) * TILES + n))

        @pl.when(i == 15)
        def _():
            for x in range(2):
                exchange(0, x).wait_send()
            gradient(4, bg, 0, TILES)
            send_terms(4)

        @pl.when(i == 16)
        def _():
            for x in range(2):
                exchange(1, x).wait_send()

        @pl.when(jnp.logical_and(i >= 16, i < 19))
        def _():
            gradient(5, bu, 3 * (i - 16), jnp.minimum(3 * (i - 15), TILES))

        @pl.when(i == 18)
        def _():
            send_terms(5)

    def wide(k, x, core):
        m = place(k // SUB)
        return pl.ds(pl.multiple_of(m * ROWS + core * HALF + x * QUARTER + lax.rem(k, SUB) * PIECE, 16), PIECE)

    def term(k, x):
        return own(k // SUB, c * HALF + x * QUARTER + lax.rem(k, SUB) * PIECE, PIECE)

    def narrow(k, x):
        m = place(k // SUB)
        return pl.ds(pl.multiple_of(m * HALF + x * QUARTER + lax.rem(k, SUB) * PIECE, 16), PIECE)

    def sum_copy(k, x):
        return pltpu.make_async_remote_copy(
            src_ref=p.at[narrow(k, x)],
            dst_ref=r.at[narrow(k, x)],
            send_sem=right_s if x == 0 else left_s,
            recv_sem=rs_r.at[x * N + k],
            device_id={"dp": dp + 2 if x == 0 else dp - 2},
            device_id_type=MESH,
        )

    def back_copy(k, x, first=False):
        return pltpu.make_async_remote_copy(
            src_ref=r.at[narrow(k, x)] if first else out.at[wide(k, x, c)],
            dst_ref=out.at[wide(k, x, c)],
            send_sem=left_s if x == 0 else right_s,
            recv_sem=ag_r.at[x * N + k],
            device_id={"dp": dp - 2 if x == 0 else dp + 2},
            device_id_type=MESH,
        )

    def share_copy(k, x, first=False):
        return pltpu.make_async_remote_copy(
            src_ref=r.at[narrow(k, x)] if first else out.at[wide(k, x, c)],
            dst_ref=out.at[wide(k, x, c)],
            send_sem=d_s,
            recv_sem=d_r.at[x * N + k],
            device_id={"dp": other},
            device_id_type=MESH,
        )

    def share_arrival(k, x):
        return pltpu.make_async_remote_copy(
            src_ref=out.at[wide(k, x, 1 - c)],
            dst_ref=out.at[wide(k, x, 1 - c)],
            send_sem=d_s,
            recv_sem=d_r.at[x * N + k],
            device_id={"dp": other},
            device_id_type=MESH,
        )

    def valid(k):
        return jnp.logical_and(k >= 0, k < N)

    def add(k, x):
        hops = z if x == 0 else LINE - 1 - z

        @pl.when(lax.rem(k, SUB) == 0)
        def _():
            exchange(k // SUB, x).wait_recv()

        mine = t[term(k, x), :].astype(jnp.float32) + p[narrow(k, x), :].astype(jnp.float32)

        @pl.when(hops == 0)
        def _():
            p[narrow(k, x), :] = mine.astype(jnp.bfloat16)
            sum_copy(k, x).start()

        @pl.when(hops > 0)
        def _():
            sum_copy(k, x).wait_recv()
            mine = t[term(k, x), :].astype(jnp.float32) + p[narrow(k, x), :].astype(jnp.float32)
            total = (mine + r[narrow(k, x), :].astype(jnp.float32)).astype(jnp.bfloat16)

            @pl.when(hops < LINE - 1)
            def _():
                p[narrow(k, x), :] = total
                sum_copy(k, x).start()

            @pl.when(hops == LINE - 1)
            def _():
                r[narrow(k, x), :] = total
                back_copy(k, x, True).start()
                share_copy(k, x, True).start()
                pltpu.make_async_copy(r.at[narrow(k, x)], out.at[wide(k, x, c)], out_s).start()
                g = total.astype(jnp.float32)
                acc[...] += jnp.sum((g * g).reshape(PIECE // 8, 8, COLS), axis=0)

    def relay(k, x):
        back_copy(k, x).wait_recv()

        @pl.when((z if x == 0 else LINE - 1 - z) > 0)
        def _():
            back_copy(k, x).start()

        share_copy(k, x).start()

    turn = SKEW * (LINE - 1)

    @pl.loop(0, N + 2 * turn + 1)
    def _(i):
        for x in range(2):
            k = i - SKEW * (z if x == 0 else LINE - 1 - z)
            pl.when(valid(k))(lambda k=k, x=x: add(k, x))
        for x in range(2):
            back = LINE - 1 - z if x == 0 else z
            k = i - turn - SKEW * back
            pl.when(jnp.logical_and(back > 0, valid(k)))(lambda k=k, x=x: relay(k, x))
            k = k - 1

            @pl.when(valid(k))
            def _(k=k, x=x):
                share_arrival(k, x).wait_recv()

        work(i)

    total = jnp.sum(acc[...])
    tile[...] = jnp.full(tile.shape, total, jnp.float32)

    def tell(slot, step):
        return pltpu.make_async_remote_copy(
            src_ref=tile, dst_ref=sq.at[slot], send_sem=sq_s.at[step - 1], recv_sem=sq_r.at[slot],
            device_id={"dp": lax.rem(dp + step, 8)}, device_id_type=MESH,
        )

    for slot, owner in enumerate((0, 1, 6, 7)):
        @pl.when(dp == owner)
        def _(slot=slot):
            for step in range(1, 8):
                tell(slot, step).start()
            sq[slot] = tile[...]

        @pl.when(dp != owner)
        def _(slot=slot):
            tell(slot, 1).wait_recv()

    squares_out[...] = sq[0] + sq[1] + sq[2] + sq[3]

    for slot, owner in enumerate((0, 1, 6, 7)):
        @pl.when(dp == owner)
        def _(slot=slot):
            for step in range(1, 8):
                tell(slot, step).wait_send()

    def all_sent(sem):
        pltpu.make_async_remote_copy(
            src_ref=p, dst_ref=p, send_sem=sem, recv_sem=xr.at[0], device_id={"dp": other}, device_id_type=MESH
        ).wait_send()

    pl.when(z < LINE - 1)(lambda: all_sent(right_s))
    pl.when(z > 0)(lambda: all_sent(left_s))
    all_sent(d_s)
    for q in range(2, MATS):
        for x in range(2):
            exchange(q, x).wait_send()

    @pl.when(jnp.logical_or(z == 0, z == LINE - 1))
    def _():
        pltpu.make_async_copy(r.at[pl.ds(0, N * PIECE)], out.at[pl.ds(0, N * PIECE)], out_s).wait()


def backward(arrays):
    dma = pltpu.SemaphoreType.DMA
    vmem = pltpu.VMEM
    return pl.pallas_call(
        backward_kernel,
        out_shape=(jax.ShapeDtypeStruct((MATS * ROWS, COLS), BF), jax.ShapeDtypeStruct((8, 128), F32)),
        in_specs=[pl.BlockSpec(memory_space=pl.ANY)] * len(arrays),
        out_specs=(pl.BlockSpec(memory_space=pl.ANY), pl.BlockSpec(memory_space=pltpu.VMEM)),
        scratch_shapes=[
            vmem((SLOTS * ROWS, COLS), BF),
            vmem((MATS * HALF, COLS), BF),
            vmem((MATS * HALF, COLS), BF),
            vmem((TOKENS, COLS), BF),
            vmem((TOKENS, COLS), BF),
            vmem((ROWS, TOKENS), BF),
            vmem((TOKENS, ROWS), BF),
            vmem((TOKENS, ROWS), BF),
            vmem((ROWS, COLS), BF),
            vmem((ROWS, COLS), BF),
            vmem((COLS, ROWS), BF),
            vmem((8, COLS), F32),
            vmem((8, 128), F32),
            vmem((4, 8, 128), F32),
            dma((13,)), dma((2 * MATS,)), dma((2 * MATS,)), dma(()), dma(()), dma((2 * N,)), dma((2 * N,)), dma(()), dma((2 * N,)), dma(()),
            dma((7,)), dma((4,)),
        ],
        compiler_params=pltpu.CompilerParams(collective_id=0, has_side_effects=True, vmem_limit_bytes=67043328),
        name="backward",
    )(*arrays)


def solution(mesh):
    def step(x, dy, *arrays):
        weights, m, v = (arrays[i : i + 3] for i in (0, 3, 6))
        x, dy = x[0], dy[0]
        kept = forward(x, dy, *weights)
        summed, squares = backward((dy, *kept, *weights))
        new = [adamw(i, squares, summed, *one) for i, one in enumerate(zip(weights, m, v, strict=True))]
        return tuple(one[which] for which in range(3) for one in new)

    return jax.shard_map(
        step,
        mesh=mesh,
        in_specs=(P(("rep", "dp"), None, None),) * 2 + (P(None, None, None),) * 9,
        out_specs=(P("rep", None, None),) * 9,
        check_vma=False,
    )
```

```python
import functools

import jax
import jax.numpy as jnp
from jax import lax
from jax.experimental import pallas as pl
from jax.experimental.pallas import tpu as pltpu
from jax.sharding import PartitionSpec as P

BF, F32 = jnp.bfloat16, jnp.float32


def dot(a, b):
    return jnp.dot(a, b, preferred_element_type=F32)


def dot_t(a, b):
    return lax.dot_general(a, b, (((1,), (1,)), ((), ())), preferred_element_type=F32)


def normed(h):
    wide = h.astype(F32)
    scale = lax.rsqrt(jnp.mean(wide**2, -1, keepdims=True) + 1e-6)
    return (wide * scale).astype(BF)


def sigmoid(x):
    return 1.0 / (1.0 + jnp.exp(-x))


def by_gate_and_up(gate, up, by_p):
    s = sigmoid(gate)
    silu = gate * s
    by_p = by_p.astype(BF).astype(F32)
    return (by_p * up * (s + silu * (1.0 - s))).astype(BF), (by_p * silu).astype(BF), (silu * up).astype(BF)


TOKENS, ROWS, COLS = 2048, 768, 1792
BLOCK = 512
TILE = 256
TILES = COLS // TILE


def forward_kernel(x, dy, w_gate, w_up, w_down, dyt_out, a0_out, a0t_out, p0_out, h1_out, a1t_out, p1_out, bg_out, bu_out, *scratch):
    weights, a1, sem = scratch[:6], scratch[6], scratch[7]
    copies = [pltpu.make_async_copy(w.at[n], weights[3 * n + i], sem.at[3 * n + i]) for n in range(2) for i, w in enumerate((w_gate, w_up, w_down))]

    first = pl.program_id(0) == 0

    @pl.when(first)
    def _():
        for copy in copies:
            copy.start()

    a0 = normed(x[...])
    a0_out[...] = a0
    a0t_out[...] = a0.T
    dyt_out[...] = dy[...].T

    def ready(*which):
        @pl.when(first)
        def _():
            for i in which:
                copies[i].wait()

    ready(0, 1)
    for n in range(TILES):
        at = slice(n * TILE, (n + 1) * TILE)
        gate, up = dot(a0_out[...], weights[0][:, at]), dot(a0_out[...], weights[1][:, at])
        p0_out[:, at] = (gate * sigmoid(gate) * up).astype(BF)
    ready(2)
    h1_out[...] = x[...] + dot(p0_out[...], weights[2][...]).astype(BF)
    a1[...] = normed(h1_out[...])
    a1t_out[...] = a1[...].T
    ready(3, 4, 5)
    for n in range(TILES):
        at = slice(n * TILE, (n + 1) * TILE)
        gate, up = dot(a1[...], weights[3][:, at]), dot(a1[...], weights[4][:, at])
        bg_out[:, at], bu_out[:, at], p1_out[:, at] = by_gate_and_up(gate, up, dot_t(dy[...], weights[5][at, :]))


def forward(x, dy, w_gate, w_up, w_down):
    narrow, wide = pl.BlockSpec((BLOCK, ROWS), lambda i: (i, 0)), pl.BlockSpec((BLOCK, COLS), lambda i: (i, 0))
    turned = pl.BlockSpec((ROWS, BLOCK), lambda i: (0, i))
    of = lambda n: jax.ShapeDtypeStruct((TOKENS, n), BF)
    of_turned = jax.ShapeDtypeStruct((ROWS, TOKENS), BF)
    return pl.pallas_call(
        forward_kernel,
        grid=(TOKENS // BLOCK,),
        out_shape=(of_turned, of(ROWS), of_turned, of(COLS), of(ROWS), of_turned, of(COLS), of(COLS), of(COLS)),
        in_specs=[narrow, narrow] + [pl.BlockSpec(memory_space=pl.ANY)] * 3,
        out_specs=(turned, narrow, turned, wide, narrow, turned, wide, wide, wide),
        scratch_shapes=[pltpu.VMEM(s, BF) for _ in range(2) for s in ((ROWS, COLS), (ROWS, COLS), (COLS, ROWS))] + [pltpu.VMEM((BLOCK, ROWS), BF), pltpu.SemaphoreType.DMA((6,))],
        compiler_params=pltpu.CompilerParams(vmem_limit_bytes=60 * 2**20),
        name="forward",
    )(x, dy, w_gate, w_up, w_down)


DEPTH = 4
CUTS = (128, 256)
BLOCKS = (2 * ROWS // CUTS[0], 2 * COLS // CUTS[1])


def adamw_kernel(squares, g_in, *refs):
    arrays = [refs[i : i + 3] for i in (0, 3, 6)]
    outs = [refs[9 + i : 18 : 3] for i in range(3)]
    rings, sems = (refs[18:25], refs[25:32]), refs[32:36]
    factor = jnp.minimum(1.0, 0.5 * lax.rsqrt(squares[...] / (2 * 3 * ROWS * COLS) + 1e-30))[0:1, 0:1]
    steps = 2 * BLOCKS[0] + BLOCKS[1]

    def copies(kind, b, inward):
        down = kind == 2
        family = 1 if down else 0
        ring, cut, per = rings[family], CUTS[family], BLOCKS[family] // 2
        slot = lax.rem(b if down else b + kind * BLOCKS[0], DEPTH)
        layer, row = b // per, pl.multiple_of(lax.rem(b, per) * cut, cut)
        at = (layer, pl.ds(row, cut))
        if not inward:
            return [pltpu.make_async_copy(ring[4 + j].at[slot], outs[kind][j].at[at], sems[2 + family].at[slot * 3 + j]) for j in range(3)]
        first = pl.multiple_of((2 * kind + layer) * ROWS, ROWS)
        g = g_in.at[pl.ds(first, ROWS), pl.ds(row, cut)] if down else g_in.at[pl.ds(pl.multiple_of(first + row, cut), cut)]
        return [
            pltpu.make_async_copy(src, ring[j].at[slot], sems[family].at[slot * 4 + j])
            for j, src in enumerate((g, *(one.at[at] for one in arrays[kind])))
        ]

    def each(b, act):
        for kind in range(3):
            lo, hi = kind * BLOCKS[0], steps if kind == 2 else (kind + 1) * BLOCKS[0]
            pl.when(jnp.logical_and(b >= lo, b < hi))(lambda kind=kind, lo=lo: act(kind, b - lo))

    def start(kind, b):
        for copy in copies(kind, b, True):
            copy.start()

    def finish(kind, b):
        for copy in copies(kind, b, False):
            copy.wait()

    def step(kind, b):
        family = 1 if kind == 2 else 0
        ring = rings[family]
        slot = lax.rem(b if kind == 2 else b + kind * BLOCKS[0], DEPTH)
        for copy in copies(kind, b, True):
            copy.wait()
        g = ring[0][slot]
        g = (g.T if kind == 2 else g).astype(F32) * factor
        m = 0.9 * ring[2][slot] + 0.1 * g
        v = 0.95 * ring[3][slot] + 0.05 * g * g
        w = ring[1][slot].astype(F32)
        ring[4][slot] = (w - 0.02 * (m * lax.rsqrt(v + 1e-8) + 0.1 * w)).astype(BF)
        ring[5][slot] = m
        ring[6][slot] = v
        for copy in copies(kind, b, False):
            copy.start()

    for b in range(DEPTH):
        start(0, b)

    @pl.loop(0, steps)
    def _(b):
        pl.when(b >= DEPTH)(lambda: each(b - DEPTH, finish))
        each(b, step)
        each(b + DEPTH, start)

    pl.loop(steps - DEPTH, steps)(lambda b: each(b, finish))


def adamw(squares, summed, weights, m, v):
    any_ = pl.BlockSpec(memory_space=pl.ANY)
    dma, vmem = pltpu.SemaphoreType.DMA, pltpu.VMEM
    ring = lambda shape, turned: [vmem((DEPTH, *(turned or shape)), BF), vmem((DEPTH, *shape), BF)] + [vmem((DEPTH, *shape), F32)] * 2 + [
        vmem((DEPTH, *shape), BF)] + [vmem((DEPTH, *shape), F32)] * 2
    return pl.pallas_call(
        adamw_kernel,
        out_shape=[jax.ShapeDtypeStruct(w.shape, dtype) for dtype in (BF, F32, F32) for w in weights],
        in_specs=[pl.BlockSpec(memory_space=vmem)] + [any_] * 10,
        out_specs=[any_] * 9,
        scratch_shapes=ring((CUTS[0], COLS), None) + ring((CUTS[1], ROWS), (ROWS, CUTS[1]))
        + [dma((DEPTH * 4,)), dma((DEPTH * 4,)), dma((DEPTH * 3,)), dma((DEPTH * 3,))],
        compiler_params=pltpu.CompilerParams(vmem_limit_bytes=60 * 2**20),
        name="adamw",
    )(squares, summed, *(one for group in zip(weights, m, v, strict=True) for one in group))


MESH = pl.DeviceIdType.MESH
MATS = 6
HALF, QUARTER = ROWS // 2, ROWS // 4
N = MATS * TILES
SKEW = 2
LEAD = 2
LINE = 4
SLOTS = 8
PART = 256


def place(q):
    return lax.rem(lax.rem(q, 3) + 2, 3) * 2 + 1 - q // 3


def backward_kernel(*refs):
    dy_in, dyt_in, a0_in, a0t_in, p0_in, h1_in, a1t_in, p1_in, bg_in, bu_in, wg_in, wu_in, wd_in = refs[:13]
    out, squares_out, t, p, r, right, rows_g, rows_u, bg, bu, lhs0, lhs1, by_h, small, wg, wu, wd, acc, tile, sq = refs[13:33]
    load, right_sem, xs, xr, right_s, left_s, rs_r, ag_r, d_s, d_r, out_s, sq_s, sq_r = refs[33:]
    dp = lax.axis_index("dp")
    z, c = dp // 2, lax.rem(dp, 2)
    other = z * 2 + 1 - c

    def fetch(src, dst, n):
        return pltpu.make_async_copy(src, dst, load.at[n])

    get_dyt, get_a1t, get_dy, get_h1, get_wd0 = fetch(dyt_in, lhs0, 0), fetch(a1t_in, lhs1, 1), fetch(dy_in, by_h, 2), fetch(h1_in, small, 3), fetch(wd_in.at[0], wd, 4)
    get_wg1, get_wu1 = fetch(wg_in.at[1], wg, 5), fetch(wu_in.at[1], wu, 6)
    get_a0, get_wg0, get_wu0, get_a0t = fetch(a0_in, small, 7), fetch(wg_in.at[0], wg, 8), fetch(wu_in.at[0], wu, 9), fetch(a0t_in, lhs1, 10)

    def get_rows(i):
        at = pl.ds(pl.multiple_of(i * PART, PART), PART)
        return fetch(bg_in.at[at], rows_g, 11), fetch(bu_in.at[at], rows_u, 12)

    def get_right(k):
        at = pl.ds(pl.multiple_of(lax.rem(k, TILES) * TILE, TILE), TILE)
        slot = lax.rem(k, 2)
        return [pltpu.make_async_copy(src.at[:, at], right.at[slot], right_sem.at[slot]) for src in (p1_in, bg_in, bu_in, p0_in)]

    def start_right(k):
        for q, copy in enumerate(get_right(k)):
            pl.when(k // TILES == q)(copy.start)

    get_dyt.start()
    for k in range(2):
        start_right(jnp.int32(k))
    for copy in (get_a1t, get_dy, get_h1, get_wg1, get_wu1, get_wd0, *get_rows(0)):
        copy.start()
    barrier = pltpu.get_barrier_semaphore()
    for step in range(1, 8):
        pl.semaphore_signal(barrier, inc=1, device_id={"dp": lax.rem(dp + step, 8)}, device_id_type=MESH)
    pl.semaphore_wait(barrier, 7)
    acc[...] = jnp.zeros_like(acc)

    def exchange(k):
        return pltpu.make_async_remote_copy(
            src_ref=t.at[lax.rem(k, SLOTS), pl.ds(pl.multiple_of((1 - c) * HALF, 16), HALF)],
            dst_ref=p.at[k],
            send_sem=xs.at[k],
            recv_sem=xr.at[k],
            device_id={"dp": other},
            device_id_type=MESH,
        )

    def gradient(k):
        q, slot = k // TILES, lax.rem(k, SLOTS)

        @pl.when(k >= SLOTS)
        def _():
            exchange(k - SLOTS).wait_send()

        @pl.when(q < 4)
        def _():
            get_right(k)[0].wait()

        at = pl.ds(pl.multiple_of(lax.rem(k, TILES) * TILE, TILE), TILE)
        for which, left, operand in (
            (jnp.logical_or(q == 0, q == 3), lhs0, lambda: right[lax.rem(k, 2)]),
            (jnp.logical_or(q == 1, q == 2), lhs1, lambda: right[lax.rem(k, 2)]),
            (q == 4, lhs1, lambda: bg[:, at]),
            (q == 5, lhs1, lambda: bu[:, at]),
        ):
            @pl.when(which)
            def _(left=left, operand=operand):
                t[slot] = dot(left[...], operand()).astype(BF)

        exchange(k).start()
        pl.when(k + 2 < 4 * TILES)(lambda: start_right(k + 2))

    get_dyt.wait()
    for k in range(LEAD):
        gradient(jnp.int32(k))

    def through_layer(i):
        at = pl.ds(pl.multiple_of(i * PART, PART), PART)
        for copy in get_rows(i):
            copy.wait()
        by_a = dot_t(rows_g[...], wg[...]).astype(BF) + dot_t(rows_u[...], wu[...]).astype(BF)

        @pl.when(i + 1 < TOKENS // PART)
        def _():
            for copy in get_rows(i + 1):
                copy.start()

        by_a, wide_h = by_a.astype(F32), small[at, :].astype(F32)
        scale = lax.rsqrt(jnp.mean(wide_h * wide_h, -1, keepdims=True) + 1e-6)
        inner = jnp.mean(by_a * wide_h, -1, keepdims=True)
        by_h[at, :] = by_h[at, :] + (by_a * scale - wide_h * (scale * scale * scale * inner)).astype(BF)

    def first_layer(i):
        rows = pl.ds(pl.multiple_of(i // TILES * BLOCK, BLOCK), BLOCK)
        at = pl.ds(pl.multiple_of(lax.rem(i, TILES) * TILE, TILE), TILE)
        gate, up = dot(small[rows, :], wg[:, at]), dot(small[rows, :], wu[:, at])
        bg[rows, at], bu[rows, at], _ = by_gate_and_up(gate, up, dot_t(by_h[rows, :], wd[at, :]))

    parts, firsts = TOKENS // PART, TOKENS // BLOCK * TILES
    THROUGH = 2
    FIRST = THROUGH + parts + 1

    def work(i):
        @pl.when(i == THROUGH)
        def _():
            for copy in (get_wg1, get_wu1, get_h1, get_dy, get_a1t):
                copy.wait()

        @pl.when(jnp.logical_and(i >= THROUGH, i < THROUGH + parts))
        def _():
            through_layer(i - THROUGH)

        @pl.when(i == THROUGH + parts - 1)
        def _():
            for copy in (get_a0, get_wg0, get_wu0):
                copy.start()

        @pl.when(jnp.logical_and(i >= THROUGH + parts, i < THROUGH + 2 * parts))
        def _():
            at = pl.ds(pl.multiple_of((i - THROUGH - parts) * PART, PART), PART)
            lhs0[:, at] = by_h[at, :].T

        @pl.when(i == FIRST)
        def _():
            for copy in (get_a0, get_wg0, get_wu0, get_wd0):
                copy.wait()

        @pl.when(jnp.logical_and(i >= FIRST, i < FIRST + firsts // 2))
        def _():
            pl.loop(0, 2)(lambda n: first_layer((i - FIRST) * 2 + n))

        @pl.when(i == 4 * TILES - LEAD)
        def _():
            get_a0t.wait()

        pl.when(i + LEAD < N)(lambda: gradient(i + LEAD))

        @pl.when(i == 3 * TILES - LEAD)
        def _():
            get_a0t.start()

    def wide(k, x, core):
        rows = pl.ds(pl.multiple_of(place(k // TILES) * ROWS + core * HALF + x * QUARTER, 16), QUARTER)
        return rows, pl.ds(pl.multiple_of(lax.rem(k, TILES) * TILE, TILE), TILE)

    def narrow(k, x):
        return k, pl.ds(x * QUARTER, QUARTER)

    def term(k, x):
        return lax.rem(k, SLOTS), pl.ds(pl.multiple_of(c * HALF + x * QUARTER, 16), QUARTER)

    def sum_copy(k, x):
        return pltpu.make_async_remote_copy(
            src_ref=p.at[narrow(k, x)],
            dst_ref=r.at[narrow(k, x)],
            send_sem=right_s if x == 0 else left_s,
            recv_sem=rs_r.at[x * N + k],
            device_id={"dp": dp + 2 if x == 0 else dp - 2},
            device_id_type=MESH,
        )

    def back_copy(k, x, first=False):
        return pltpu.make_async_remote_copy(
            src_ref=r.at[narrow(k, x)] if first else out.at[wide(k, x, c)],
            dst_ref=out.at[wide(k, x, c)],
            send_sem=left_s if x == 0 else right_s,
            recv_sem=ag_r.at[x * N + k],
            device_id={"dp": dp - 2 if x == 0 else dp + 2},
            device_id_type=MESH,
        )

    def share_copy(k, x, first=False):
        return pltpu.make_async_remote_copy(
            src_ref=r.at[narrow(k, x)] if first else out.at[wide(k, x, c)],
            dst_ref=out.at[wide(k, x, c)],
            send_sem=d_s,
            recv_sem=d_r.at[x * N + k],
            device_id={"dp": other},
            device_id_type=MESH,
        )

    def share_arrival(k, x):
        return pltpu.make_async_remote_copy(
            src_ref=out.at[wide(k, x, 1 - c)],
            dst_ref=out.at[wide(k, x, 1 - c)],
            send_sem=d_s,
            recv_sem=d_r.at[x * N + k],
            device_id={"dp": other},
            device_id_type=MESH,
        )

    def valid(k):
        return jnp.logical_and(k >= 0, k < N)

    def add(k, x):
        hops = z if x == 0 else LINE - 1 - z

        first = z < LINE // 2 if x == 0 else z >= LINE // 2
        pl.when(first)(lambda: exchange(k).wait_recv())

        @pl.when(hops == 0)
        def _():
            mine = t[term(k, x)].astype(jnp.float32) + p[narrow(k, x)].astype(jnp.float32)
            p[narrow(k, x)] = mine.astype(jnp.bfloat16)
            sum_copy(k, x).start()

        @pl.when(hops > 0)
        def _():
            sum_copy(k, x).wait_recv()
            mine = t[term(k, x)].astype(jnp.float32) + p[narrow(k, x)].astype(jnp.float32)
            total = (mine + r[narrow(k, x)].astype(jnp.float32)).astype(jnp.bfloat16)

            @pl.when(hops < LINE - 1)
            def _():
                p[narrow(k, x)] = total
                sum_copy(k, x).start()

            @pl.when(hops == LINE - 1)
            def _():
                r[narrow(k, x)] = total
                back_copy(k, x, True).start()
                share_copy(k, x, True).start()
                pltpu.make_async_copy(r.at[narrow(k, x)], out.at[wide(k, x, c)], out_s).start()
                g = total.astype(jnp.float32)
                acc[...] += jnp.sum((g * g).reshape(QUARTER // 8, 8, TILE), axis=0)

    def relay(k, x):
        back_copy(k, x).wait_recv()

        @pl.when((z if x == 0 else LINE - 1 - z) > 0)
        def _():
            back_copy(k, x).start()

        share_copy(k, x).start()

    turn = SKEW * (LINE - 1)

    @pl.loop(0, N + 2 * turn + 1)
    def _(i):
        for x in range(2):
            k = i - SKEW * (z if x == 0 else LINE - 1 - z)
            pl.when(valid(k))(lambda k=k, x=x: add(k, x))
        for x in range(2):
            back = LINE - 1 - z if x == 0 else z
            k = i - turn - SKEW * back
            pl.when(jnp.logical_and(back > 0, valid(k)))(lambda k=k, x=x: relay(k, x))
            k = k - 1

            @pl.when(valid(k))
            def _(k=k, x=x):
                share_arrival(k, x).wait_recv()

        work(i)

    total = jnp.sum(acc[...])
    tile[...] = jnp.full(tile.shape, total, jnp.float32)

    def tell(slot, step):
        return pltpu.make_async_remote_copy(
            src_ref=tile, dst_ref=sq.at[slot], send_sem=sq_s.at[step - 1], recv_sem=sq_r.at[slot],
            device_id={"dp": lax.rem(dp + step, 8)}, device_id_type=MESH,
        )

    for slot, owner in enumerate((0, 1, 6, 7)):
        @pl.when(dp == owner)
        def _(slot=slot):
            for step in range(1, 8):
                tell(slot, step).start()
            sq[slot] = tile[...]

        @pl.when(dp != owner)
        def _(slot=slot):
            tell(slot, 1).wait_recv()

    squares_out[...] = sq[0] + sq[1] + sq[2] + sq[3]

    for slot, owner in enumerate((0, 1, 6, 7)):
        @pl.when(dp == owner)
        def _(slot=slot):
            for step in range(1, 8):
                tell(slot, step).wait_send()

    half = pl.ds(0, N // 2)

    def all_sent(sem):
        pltpu.make_async_remote_copy(src_ref=p, dst_ref=p, send_sem=sem, recv_sem=xr.at[0], device_id={"dp": other}, device_id_type=MESH).wait_send()

    pl.when(z < LINE - 1)(lambda: all_sent(right_s))
    pl.when(z > 0)(lambda: all_sent(left_s))
    all_sent(d_s)
    pl.loop(N - SLOTS, N)(lambda k: exchange(k).wait_send())

    @pl.when(jnp.logical_or(z == 0, z == LINE - 1))
    def _():
        pltpu.make_async_copy(r.at[half], p.at[half], out_s).wait()


def backward(arrays):
    dma = pltpu.SemaphoreType.DMA
    vmem = pltpu.VMEM
    return pl.pallas_call(
        backward_kernel,
        out_shape=(jax.ShapeDtypeStruct((MATS * ROWS, COLS), BF), jax.ShapeDtypeStruct((8, 128), F32)),
        in_specs=[pl.BlockSpec(memory_space=pl.ANY)] * len(arrays),
        out_specs=(pl.BlockSpec(memory_space=pl.ANY), pl.BlockSpec(memory_space=pltpu.VMEM)),
        scratch_shapes=[
            vmem((SLOTS, ROWS, TILE), BF),
            vmem((N, HALF, TILE), BF),
            vmem((N, HALF, TILE), BF),
            vmem((2, TOKENS, TILE), BF),
            vmem((PART, COLS), BF),
            vmem((PART, COLS), BF),
            vmem((TOKENS, COLS), BF),
            vmem((TOKENS, COLS), BF),
            vmem((ROWS, TOKENS), BF),
            vmem((ROWS, TOKENS), BF),
            vmem((TOKENS, ROWS), BF),
            vmem((TOKENS, ROWS), BF),
            vmem((ROWS, COLS), BF),
            vmem((ROWS, COLS), BF),
            vmem((COLS, ROWS), BF),
            vmem((8, TILE), F32),
            vmem((8, 128), F32),
            vmem((4, 8, 128), F32),
            dma((13,)), dma((2,)), dma((N,)), dma((N,)), dma(()), dma(()), dma((2 * N,)), dma((2 * N,)), dma(()), dma((2 * N,)), dma(()),
            dma((7,)), dma((4,)),
        ],
        compiler_params=pltpu.CompilerParams(collective_id=0, has_side_effects=True, vmem_limit_bytes=67043328),
        name="backward",
    )(*arrays)


def solution(mesh):
    def step(x, dy, *arrays):
        weights, m, v = (arrays[i : i + 3] for i in (0, 3, 6))
        x, dy = x[0], dy[0]
        kept = forward(x, dy, *weights)
        summed, squares = backward((dy, *kept, *weights))
        return tuple(adamw(squares, summed, weights, m, v))

    return jax.shard_map(
        step,
        mesh=mesh,
        in_specs=(P(("rep", "dp"), None, None),) * 2 + (P(None, None, None),) * 9,
        out_specs=(P("rep", None, None),) * 9,
        check_vma=False,
    )
```

```python
import functools

import jax
import jax.numpy as jnp
from jax import lax
from jax.experimental import pallas as pl
from jax.experimental.pallas import tpu as pltpu
from jax.sharding import PartitionSpec as P

BF, F32 = jnp.bfloat16, jnp.float32


def dot(a, b):
    return jnp.dot(a, b, preferred_element_type=F32)


def dot_t(a, b):
    return lax.dot_general(a, b, (((1,), (1,)), ((), ())), preferred_element_type=F32)


def normed(h):
    wide = h.astype(F32)
    scale = lax.rsqrt(jnp.mean(wide**2, -1, keepdims=True) + 1e-6)
    return (wide * scale).astype(BF)


def sigmoid(x):
    return 1.0 / (1.0 + jnp.exp(-x))


def by_gate_and_up(gate, up, by_p):
    s = sigmoid(gate)
    silu = gate * s
    by_p = by_p.astype(BF).astype(F32)
    return (by_p * up * (s + silu * (1.0 - s))).astype(BF), (by_p * silu).astype(BF), (silu * up).astype(BF)


TOKENS, ROWS, COLS = 2048, 768, 1792
BLOCK = 512
TILE = 256
TILES = COLS // TILE


def forward_kernel(x, dy, w_gate, w_up, w_down, dyt_out, a0_out, a0t_out, p0_out, h1_out, a1t_out, p1_out, bg_out, bu_out, *scratch):
    weights, a1, sem = scratch[:6], scratch[6], scratch[7]
    copies = [pltpu.make_async_copy(w.at[n], weights[3 * n + i], sem.at[3 * n + i]) for n in range(2) for i, w in enumerate((w_gate, w_up, w_down))]

    first = pl.program_id(0) == 0

    @pl.when(first)
    def _():
        for copy in copies:
            copy.start()

    a0 = normed(x[...])
    a0_out[...] = a0
    a0t_out[...] = a0.T
    dyt_out[...] = dy[...].T

    def ready(*which):
        @pl.when(first)
        def _():
            for i in which:
                copies[i].wait()

    ready(0, 1)
    tiles = [slice(n * TILE, (n + 1) * TILE) for n in range(TILES)]

    def pipelined(matmuls, rest):
        last = None
        for at in tiles:
            now = matmuls(at)
            if last is not None:
                rest(*last)
            last = at, now
        rest(*last)

    def product(at, two):
        p0_out[:, at] = (two[0] * sigmoid(two[0]) * two[1]).astype(BF)

    pipelined(lambda at: (dot(a0_out[...], weights[0][:, at]), dot(a0_out[...], weights[1][:, at])), product)
    ready(2)
    h1_out[...] = x[...] + dot(p0_out[...], weights[2][...]).astype(BF)
    a1[...] = normed(h1_out[...])
    a1t_out[...] = a1[...].T
    ready(3, 4, 5)

    def cotangents(at, three):
        bg_out[:, at], bu_out[:, at], p1_out[:, at] = by_gate_and_up(*three)

    pipelined(lambda at: (dot(a1[...], weights[3][:, at]), dot(a1[...], weights[4][:, at]), dot_t(dy[...], weights[5][at, :])), cotangents)


def forward(x, dy, w_gate, w_up, w_down):
    narrow, wide = pl.BlockSpec((BLOCK, ROWS), lambda i: (i, 0)), pl.BlockSpec((BLOCK, COLS), lambda i: (i, 0))
    turned = pl.BlockSpec((ROWS, BLOCK), lambda i: (0, i))
    of = lambda n: jax.ShapeDtypeStruct((TOKENS, n), BF)
    of_turned = jax.ShapeDtypeStruct((ROWS, TOKENS), BF)
    return pl.pallas_call(
        forward_kernel,
        grid=(TOKENS // BLOCK,),
        out_shape=(of_turned, of(ROWS), of_turned, of(COLS), of(ROWS), of_turned, of(COLS), of(COLS), of(COLS)),
        in_specs=[narrow, narrow] + [pl.BlockSpec(memory_space=pl.ANY)] * 3,
        out_specs=(turned, narrow, turned, wide, narrow, turned, wide, wide, wide),
        scratch_shapes=[pltpu.VMEM(s, BF) for _ in range(2) for s in ((ROWS, COLS), (ROWS, COLS), (COLS, ROWS))] + [pltpu.VMEM((BLOCK, ROWS), BF), pltpu.SemaphoreType.DMA((6,))],
        compiler_params=pltpu.CompilerParams(vmem_limit_bytes=60 * 2**20),
        name="forward",
    )(x, dy, w_gate, w_up, w_down)


DEPTH = 4
CUTS = (128, 256)
BLOCKS = (2 * ROWS // CUTS[0], 2 * COLS // CUTS[1])


def adamw_kernel(squares, g_in, *refs):
    arrays = [refs[i : i + 3] for i in (0, 3, 6)]
    outs = [refs[9 + i : 18 : 3] for i in range(3)]
    rings, sems = (refs[18:25], refs[25:32]), refs[32:36]
    factor = jnp.minimum(1.0, 0.5 * lax.rsqrt(squares[...] / (2 * 3 * ROWS * COLS) + 1e-30))[0:1, 0:1]
    steps = 2 * BLOCKS[0] + BLOCKS[1]

    def copies(kind, b, inward):
        down = kind == 2
        family = 1 if down else 0
        ring, cut, per = rings[family], CUTS[family], BLOCKS[family] // 2
        slot = lax.rem(b if down else b + kind * BLOCKS[0], DEPTH)
        layer, row = b // per, pl.multiple_of(lax.rem(b, per) * cut, cut)
        at = (layer, pl.ds(row, cut))
        if not inward:
            return [pltpu.make_async_copy(ring[4 + j].at[slot], outs[kind][j].at[at], sems[2 + family].at[slot * 3 + j]) for j in range(3)]
        first = pl.multiple_of((2 * kind + layer) * ROWS, ROWS)
        g = g_in.at[pl.ds(first, ROWS), pl.ds(row, cut)] if down else g_in.at[pl.ds(pl.multiple_of(first + row, cut), cut)]
        return [
            pltpu.make_async_copy(src, ring[j].at[slot], sems[family].at[slot * 4 + j])
            for j, src in enumerate((g, *(one.at[at] for one in arrays[kind])))
        ]

    def each(b, act):
        for kind in range(3):
            lo, hi = kind * BLOCKS[0], steps if kind == 2 else (kind + 1) * BLOCKS[0]
            pl.when(jnp.logical_and(b >= lo, b < hi))(lambda kind=kind, lo=lo: act(kind, b - lo))

    def start(kind, b):
        for copy in copies(kind, b, True):
            copy.start()

    def finish(kind, b):
        for copy in copies(kind, b, False):
            copy.wait()

    def step(kind, b):
        family = 1 if kind == 2 else 0
        ring = rings[family]
        slot = lax.rem(b if kind == 2 else b + kind * BLOCKS[0], DEPTH)
        for copy in copies(kind, b, True):
            copy.wait()
        g = ring[0][slot]
        g = (g.T if kind == 2 else g).astype(F32) * factor
        m = 0.9 * ring[2][slot] + 0.1 * g
        v = 0.95 * ring[3][slot] + 0.05 * g * g
        w = ring[1][slot].astype(F32)
        ring[4][slot] = (w - 0.02 * (m * lax.rsqrt(v + 1e-8) + 0.1 * w)).astype(BF)
        ring[5][slot] = m
        ring[6][slot] = v
        for copy in copies(kind, b, False):
            copy.start()

    for b in range(DEPTH):
        start(0, b)

    @pl.loop(0, steps)
    def _(b):
        pl.when(b >= DEPTH)(lambda: each(b - DEPTH, finish))
        each(b, step)
        each(b + DEPTH, start)

    pl.loop(steps - DEPTH, steps)(lambda b: each(b, finish))


def adamw(squares, summed, weights, m, v):
    any_ = pl.BlockSpec(memory_space=pl.ANY)
    dma, vmem = pltpu.SemaphoreType.DMA, pltpu.VMEM
    ring = lambda shape, turned: [vmem((DEPTH, *(turned or shape)), BF), vmem((DEPTH, *shape), BF)] + [vmem((DEPTH, *shape), F32)] * 2 + [
        vmem((DEPTH, *shape), BF)] + [vmem((DEPTH, *shape), F32)] * 2
    return pl.pallas_call(
        adamw_kernel,
        out_shape=[jax.ShapeDtypeStruct(w.shape, dtype) for dtype in (BF, F32, F32) for w in weights],
        in_specs=[pl.BlockSpec(memory_space=vmem)] + [any_] * 10,
        out_specs=[any_] * 9,
        scratch_shapes=ring((CUTS[0], COLS), None) + ring((CUTS[1], ROWS), (ROWS, CUTS[1]))
        + [dma((DEPTH * 4,)), dma((DEPTH * 4,)), dma((DEPTH * 3,)), dma((DEPTH * 3,))],
        compiler_params=pltpu.CompilerParams(vmem_limit_bytes=60 * 2**20),
        name="adamw",
    )(squares, summed, *(one for group in zip(weights, m, v, strict=True) for one in group))


MESH = pl.DeviceIdType.MESH
MATS = 6
HALF, QUARTER = ROWS // 2, ROWS // 4
N = MATS * TILES
PIECES = 2 * N
SKEW = 3
LEAD = 2
RING = 16
LINE = 4
SLOTS = 8
PART = 256


def place(q):
    return lax.rem(lax.rem(q, 3) + 2, 3) * 2 + 1 - q // 3


def backward_kernel(*refs):
    dy_in, dyt_in, a0_in, a0t_in, p0_in, h1_in, a1t_in, p1_in, bg_in, bu_in, wg_in, wu_in, wd_in = refs[:13]
    out, squares_out, t, p, done, arrived, swapped, right, rows_g, rows_u, bg, bu, lhs0, lhs1, by_h, small, wg, wu, wd, acc, tile, sq = refs[13:35]
    load, right_sem, xs, xr, sent, got, swap_got, back_sent, d_s, d_r, out_s, sq_s, sq_r = refs[35:]
    dp = lax.axis_index("dp")
    z, c = dp // 2, lax.rem(dp, 2)
    other = z * 2 + 1 - c
    outer = jnp.logical_or(z == 0, z == LINE - 1)
    partner = lax.select(z < LINE // 2, 1 - z, 5 - z) * 2 + c
    across = (LINE - 1 - z) * 2 + c

    def fetch(src, dst, n):
        return pltpu.make_async_copy(src, dst, load.at[n])

    get_dyt, get_a1t, get_dy, get_h1, get_wd0 = fetch(dyt_in, lhs0, 0), fetch(a1t_in, lhs1, 1), fetch(dy_in, by_h, 2), fetch(h1_in, small, 3), fetch(wd_in.at[0], wd, 4)
    get_wg1, get_wu1 = fetch(wg_in.at[1], wg, 5), fetch(wu_in.at[1], wu, 6)
    get_a0, get_wg0, get_wu0, get_a0t = fetch(a0_in, small, 7), fetch(wg_in.at[0], wg, 8), fetch(wu_in.at[0], wu, 9), fetch(a0t_in, lhs1, 10)

    def get_rows(i):
        at = pl.ds(pl.multiple_of(i * PART, PART), PART)
        return fetch(bg_in.at[at], rows_g, 11), fetch(bu_in.at[at], rows_u, 12)

    def get_right(k):
        at = pl.ds(pl.multiple_of(lax.rem(k, TILES) * TILE, TILE), TILE)
        slot = lax.rem(k, 2)
        return [pltpu.make_async_copy(src.at[:, at], right.at[slot], right_sem.at[slot]) for src in (p1_in, bg_in, bu_in, p0_in)]

    def start_right(k):
        for q, copy in enumerate(get_right(k)):
            pl.when(k // TILES == q)(copy.start)

    get_dyt.start()
    for k in range(2):
        start_right(jnp.int32(k))
    for copy in (get_a1t, get_dy, get_h1, get_wg1, get_wu1, get_wd0, *get_rows(0)):
        copy.start()
    barrier = pltpu.get_barrier_semaphore()
    for step in range(1, 8):
        pl.semaphore_signal(barrier, inc=1, device_id={"dp": lax.rem(dp + step, 8)}, device_id_type=MESH)
    pl.semaphore_wait(barrier, 7)
    acc[...] = jnp.zeros_like(acc)

    def exchange(k):
        return pltpu.make_async_remote_copy(
            src_ref=t.at[lax.rem(k, SLOTS), pl.ds(pl.multiple_of((1 - c) * HALF, 16), HALF)],
            dst_ref=p.at[k],
            send_sem=xs.at[k],
            recv_sem=xr.at[k],
            device_id={"dp": other},
            device_id_type=MESH,
        )

    def gradient(k):
        q, slot = k // TILES, lax.rem(k, SLOTS)

        @pl.when(k >= SLOTS)
        def _():
            exchange(k - SLOTS).wait_send()

        @pl.when(q < 4)
        def _():
            get_right(k)[0].wait()

        at = pl.ds(pl.multiple_of(lax.rem(k, TILES) * TILE, TILE), TILE)
        for which, left, operand in (
            (jnp.logical_or(q == 0, q == 3), lhs0, lambda: right[lax.rem(k, 2)]),
            (jnp.logical_or(q == 1, q == 2), lhs1, lambda: right[lax.rem(k, 2)]),
            (q == 4, lhs1, lambda: bg[:, at]),
            (q == 5, lhs1, lambda: bu[:, at]),
        ):
            @pl.when(which)
            def _(left=left, operand=operand):
                t[slot] = dot(left[...], operand()).astype(BF)

        exchange(k).start()
        pl.when(k + 2 < 4 * TILES)(lambda: start_right(k + 2))

    get_dyt.wait()
    for k in range(LEAD):
        gradient(jnp.int32(k))

    def through_layer(i):
        at = pl.ds(pl.multiple_of(i * PART, PART), PART)
        for copy in get_rows(i):
            copy.wait()
        by_a = dot_t(rows_g[...], wg[...]).astype(BF) + dot_t(rows_u[...], wu[...]).astype(BF)

        @pl.when(i + 1 < TOKENS // PART)
        def _():
            for copy in get_rows(i + 1):
                copy.start()

        by_a, wide_h = by_a.astype(F32), small[at, :].astype(F32)
        scale = lax.rsqrt(jnp.mean(wide_h * wide_h, -1, keepdims=True) + 1e-6)
        inner = jnp.mean(by_a * wide_h, -1, keepdims=True)
        by_h[at, :] = by_h[at, :] + (by_a * scale - wide_h * (scale * scale * scale * inner)).astype(BF)

    def first_layer(i):
        rows = pl.ds(pl.multiple_of(i // TILES * BLOCK, BLOCK), BLOCK)
        at = pl.ds(pl.multiple_of(lax.rem(i, TILES) * TILE, TILE), TILE)
        gate, up = dot(small[rows, :], wg[:, at]), dot(small[rows, :], wu[:, at])
        bg[rows, at], bu[rows, at], _ = by_gate_and_up(gate, up, dot_t(by_h[rows, :], wd[at, :]))

    parts, firsts = TOKENS // PART, TOKENS // BLOCK * TILES
    THROUGH = 2
    TURN = THROUGH + parts
    FIRST = 2 * TURN + 2

    def work(i):
        turn, even = i // 2, lax.rem(i, 2) == 0

        @pl.when(i == 2 * THROUGH)
        def _():
            for copy in (get_wg1, get_wu1, get_h1, get_dy, get_a1t):
                copy.wait()

        @pl.when(jnp.logical_and(even, jnp.logical_and(turn >= THROUGH, turn < TURN)))
        def _():
            through_layer(turn - THROUGH)

        @pl.when(i == 2 * TURN - 1)
        def _():
            for copy in (get_a0, get_wg0, get_wu0):
                copy.start()

        @pl.when(jnp.logical_and(even, jnp.logical_and(turn >= TURN, turn < TURN + parts)))
        def _():
            at = pl.ds(pl.multiple_of((turn - TURN) * PART, PART), PART)
            lhs0[:, at] = by_h[at, :].T

        @pl.when(i == FIRST)
        def _():
            for copy in (get_a0, get_wg0, get_wu0, get_wd0):
                copy.wait()

        @pl.when(jnp.logical_and(i >= FIRST, i < FIRST + firsts))
        def _():
            first_layer(i - FIRST)

        @pl.when(i == 2 * (4 * TILES - LEAD))
        def _():
            get_a0t.wait()

        pl.when(jnp.logical_and(jnp.logical_not(even), turn + LEAD < N))(lambda: gradient(turn + LEAD))

        @pl.when(i == 2 * (3 * TILES - LEAD))
        def _():
            get_a0t.start()

    def wide(h, core):
        k = h // 2
        rows = pl.ds(pl.multiple_of(place(k // TILES) * ROWS + core * HALF + lax.rem(h, 2) * QUARTER, 16), QUARTER)
        return rows, pl.ds(pl.multiple_of(lax.rem(k, TILES) * TILE, TILE), TILE)

    def narrow(h):
        return h // 2, pl.ds(pl.multiple_of(lax.rem(h, 2) * QUARTER, 16), QUARTER)

    def remote(src, dst, send_sem, recv_sem, to):
        return pltpu.make_async_remote_copy(
            src_ref=src, dst_ref=dst, send_sem=send_sem, recv_sem=recv_sem, device_id={"dp": to}, device_id_type=MESH
        )

    def inward(h):
        return remote(p.at[narrow(h)], arrived.at[lax.rem(h, RING)], sent, got.at[h], partner)

    def swap(h):
        return remote(p.at[narrow(h)], swapped.at[lax.rem(h, RING)], sent, swap_got.at[h], across)

    def outward(h):
        return remote(done.at[narrow(h)], out.at[wide(h, c)], back_sent, got.at[h], partner)

    def share(h, first):
        return remote(done.at[narrow(h)] if first else out.at[wide(h, c)], out.at[wide(h, c)], d_s, d_r, other)

    def mine(h):
        k = h // 2
        pl.when(lax.rem(h, 2) == 0)(lambda: exchange(k).wait_recv())
        own = t[lax.rem(k, SLOTS), pl.ds(pl.multiple_of(c * HALF + lax.rem(h, 2) * QUARTER, 16), QUARTER)]
        return own.astype(F32) + p[narrow(h)].astype(F32)

    def valid(h):
        return jnp.logical_and(h >= 0, h < PIECES)

    def send_in(h):
        p[narrow(h)] = mine(h).astype(BF)
        inward(h).start()

    def add_and_swap(h):
        total = mine(h)
        inward(h).wait_recv()
        p[narrow(h)] = (total + arrived[lax.rem(h, RING)].astype(F32)).astype(BF)
        swap(h).start()

    def finish(h):
        swap(h).wait_recv()
        g = (p[narrow(h)].astype(F32) + swapped[lax.rem(h, RING)].astype(F32)).astype(BF)
        done[narrow(h)] = g
        outward(h).start()
        share(h, True).start()
        pltpu.make_async_copy(done.at[narrow(h)], out.at[wide(h, c)], out_s).start()
        g = g.astype(F32)
        acc[...] += jnp.sum((g * g).reshape(QUARTER // 8, 8, TILE), axis=0)

    def take(h):
        outward(h).wait_recv()
        share(h, False).start()

    @pl.loop(0, PIECES + 3 * SKEW)
    def _(i):
        @pl.when(outer)
        def _():
            pl.when(valid(i - 3 * SKEW))(lambda: take(i - 3 * SKEW))
            pl.when(valid(i))(lambda: send_in(i))

        @pl.when(jnp.logical_not(outer))
        def _():
            pl.when(valid(i - 2 * SKEW))(lambda: finish(i - 2 * SKEW))
            pl.when(valid(i - SKEW))(lambda: add_and_swap(i - SKEW))

        work(i)

    total = jnp.sum(acc[...])
    tile[...] = jnp.full(tile.shape, total, jnp.float32)

    def tell(slot, step):
        return pltpu.make_async_remote_copy(
            src_ref=tile, dst_ref=sq.at[slot], send_sem=sq_s.at[step - 1], recv_sem=sq_r.at[slot],
            device_id={"dp": lax.rem(dp + step, 8)}, device_id_type=MESH,
        )

    for slot, owner in enumerate((2, 3)):
        @pl.when(dp == owner)
        def _(slot=slot):
            for step in range(1, 8):
                tell(slot, step).start()
            sq[slot] = tile[...]

        @pl.when(dp != owner)
        def _(slot=slot):
            tell(slot, 1).wait_recv()

    squares_out[...] = sq[0] + sq[1]

    for slot, owner in enumerate((2, 3)):
        @pl.when(dp == owner)
        def _(slot=slot):
            for step in range(1, 8):
                tell(slot, step).wait_send()

    remote(p, p, sent, got.at[0], other).wait_send()
    remote(p, p, d_s, d_r, other).wait()
    pl.loop(N - SLOTS, N)(lambda k: exchange(k).wait_send())

    @pl.when(jnp.logical_not(outer))
    def _():
        remote(p, p, back_sent, got.at[0], other).wait_send()
        pltpu.make_async_copy(done, p, out_s).wait()


def backward(arrays):
    dma = pltpu.SemaphoreType.DMA
    vmem = pltpu.VMEM
    return pl.pallas_call(
        backward_kernel,
        out_shape=(jax.ShapeDtypeStruct((MATS * ROWS, COLS), BF), jax.ShapeDtypeStruct((8, 128), F32)),
        in_specs=[pl.BlockSpec(memory_space=pl.ANY)] * len(arrays),
        out_specs=(pl.BlockSpec(memory_space=pl.ANY), pl.BlockSpec(memory_space=pltpu.VMEM)),
        scratch_shapes=[
            vmem((SLOTS, ROWS, TILE), BF),
            vmem((N, HALF, TILE), BF),
            vmem((N, HALF, TILE), BF),
            vmem((RING, QUARTER, TILE), BF),
            vmem((RING, QUARTER, TILE), BF),
            vmem((2, TOKENS, TILE), BF),
            vmem((PART, COLS), BF),
            vmem((PART, COLS), BF),
            vmem((TOKENS, COLS), BF),
            vmem((TOKENS, COLS), BF),
            vmem((ROWS, TOKENS), BF),
            vmem((ROWS, TOKENS), BF),
            vmem((TOKENS, ROWS), BF),
            vmem((TOKENS, ROWS), BF),
            vmem((ROWS, COLS), BF),
            vmem((ROWS, COLS), BF),
            vmem((COLS, ROWS), BF),
            vmem((8, TILE), F32),
            vmem((8, 128), F32),
            vmem((2, 8, 128), F32),
            dma((13,)), dma((2,)), dma((N,)), dma((N,)), dma(()), dma((PIECES,)), dma((PIECES,)), dma(()), dma(()), dma(()), dma(()),
            dma((7,)), dma((2,)),
        ],
        compiler_params=pltpu.CompilerParams(collective_id=0, has_side_effects=True, vmem_limit_bytes=67043328),
        name="backward",
    )(*arrays)


def solution(mesh):
    def step(x, dy, *arrays):
        weights, m, v = (arrays[i : i + 3] for i in (0, 3, 6))
        x, dy = x[0], dy[0]
        kept = forward(x, dy, *weights)
        summed, squares = backward((dy, *kept, *weights))
        return tuple(adamw(squares, summed, weights, m, v))

    return jax.shard_map(
        step,
        mesh=mesh,
        in_specs=(P(("rep", "dp"), None, None),) * 2 + (P(None, None, None),) * 9,
        out_specs=(P("rep", None, None),) * 9,
        check_vma=False,
    )
```

```python
import functools

import jax
import jax.numpy as jnp
from jax import lax
from jax.experimental import pallas as pl
from jax.experimental.pallas import tpu as pltpu
from jax.sharding import PartitionSpec as P

BF, F32 = jnp.bfloat16, jnp.float32


def dot(a, b):
    return jnp.dot(a, b, preferred_element_type=F32)


def dot_t(a, b):
    return lax.dot_general(a, b, (((1,), (1,)), ((), ())), preferred_element_type=F32)


def normed(h):
    wide = h.astype(F32)
    scale = lax.rsqrt(jnp.mean(wide**2, -1, keepdims=True) + 1e-6)
    return (wide * scale).astype(BF)


def sigmoid(x):
    return 1.0 / (1.0 + jnp.exp(-x))


def by_gate_and_up(gate, up, by_p):
    s = sigmoid(gate)
    silu = gate * s
    by_p = by_p.astype(BF).astype(F32)
    return (by_p * up * (s + silu * (1.0 - s))).astype(BF), (by_p * silu).astype(BF), (silu * up).astype(BF)


TOKENS, ROWS, COLS = 2048, 768, 1792
BLOCK = 512
TILE = 256
TILES = COLS // TILE


def forward_kernel(x, dy, w_gate, w_up, w_down, dyt_out, a0_out, p0_out, h1_out, a1t_out, p1_out, bg_out, bu_out, *scratch):
    weights, a1, sem = scratch[:6], scratch[6], scratch[7]
    copies = [pltpu.make_async_copy(w.at[n], weights[3 * n + i], sem.at[3 * n + i]) for n in range(2) for i, w in enumerate((w_gate, w_up, w_down))]

    first = pl.program_id(0) == 0

    @pl.when(first)
    def _():
        for copy in copies:
            copy.start()

    a0 = normed(x[...])
    a0_out[...] = a0
    dyt_out[...] = dy[...].T

    def ready(*which):
        @pl.when(first)
        def _():
            for i in which:
                copies[i].wait()

    ready(0, 1)
    tiles = [slice(n * TILE, (n + 1) * TILE) for n in range(TILES)]

    def pipelined(matmuls, rest):
        last = None
        for at in tiles:
            now = matmuls(at)
            if last is not None:
                rest(*last)
            last = at, now
        rest(*last)

    def product(at, two):
        p0_out[:, at] = (two[0] * sigmoid(two[0]) * two[1]).astype(BF)

    pipelined(lambda at: (dot(a0_out[...], weights[0][:, at]), dot(a0_out[...], weights[1][:, at])), product)
    ready(2)
    h1_out[...] = x[...] + dot(p0_out[...], weights[2][...]).astype(BF)
    a1[...] = normed(h1_out[...])
    a1t_out[...] = a1[...].T
    ready(3, 4, 5)

    def cotangents(at, three):
        bg_out[:, at], bu_out[:, at], p1_out[:, at] = by_gate_and_up(*three)

    pipelined(lambda at: (dot(a1[...], weights[3][:, at]), dot(a1[...], weights[4][:, at]), dot_t(dy[...], weights[5][at, :])), cotangents)


def forward(x, dy, w_gate, w_up, w_down):
    narrow, wide = pl.BlockSpec((BLOCK, ROWS), lambda i: (i, 0)), pl.BlockSpec((BLOCK, COLS), lambda i: (i, 0))
    turned = pl.BlockSpec((ROWS, BLOCK), lambda i: (0, i))
    of = lambda n: jax.ShapeDtypeStruct((TOKENS, n), BF)
    of_turned = jax.ShapeDtypeStruct((ROWS, TOKENS), BF)
    return pl.pallas_call(
        forward_kernel,
        grid=(TOKENS // BLOCK,),
        out_shape=(of_turned, of(ROWS), of(COLS), of(ROWS), of_turned, of(COLS), of(COLS), of(COLS)),
        in_specs=[narrow, narrow] + [pl.BlockSpec(memory_space=pl.ANY)] * 3,
        out_specs=(turned, narrow, wide, narrow, turned, wide, wide, wide),
        scratch_shapes=[pltpu.VMEM(s, BF) for _ in range(2) for s in ((ROWS, COLS), (ROWS, COLS), (COLS, ROWS))] + [pltpu.VMEM((BLOCK, ROWS), BF), pltpu.SemaphoreType.DMA((6,))],
        compiler_params=pltpu.CompilerParams(vmem_limit_bytes=60 * 2**20),
        name="forward",
    )(x, dy, w_gate, w_up, w_down)


DEPTH = 8
CUTS = (64, 128)
BLOCKS = (2 * ROWS // CUTS[0], 2 * COLS // CUTS[1])


def adamw_kernel(squares, g_in, *refs):
    arrays = [refs[i : i + 3] for i in (0, 3, 6)]
    outs = [refs[9 + i : 18 : 3] for i in range(3)]
    rings, sems = (refs[18:25], refs[25:32]), refs[32:36]
    factor = jnp.minimum(1.0, 0.5 * lax.rsqrt(squares[...] / (2 * 3 * ROWS * COLS) + 1e-30))[0:1, 0:1]
    steps = 2 * BLOCKS[0] + BLOCKS[1]

    def copies(kind, b, inward):
        down = kind == 2
        family = 1 if down else 0
        ring, cut, per = rings[family], CUTS[family], BLOCKS[family] // 2
        slot = lax.rem(b if down else b + kind * BLOCKS[0], DEPTH)
        layer, row = b // per, pl.multiple_of(lax.rem(b, per) * cut, cut)
        at = (layer, pl.ds(row, cut))
        if not inward:
            return [pltpu.make_async_copy(ring[4 + j].at[slot], outs[kind][j].at[at], sems[2 + family].at[slot * 3 + j]) for j in range(3)]
        first = pl.multiple_of((2 * kind + layer) * ROWS, ROWS)
        g = g_in.at[pl.ds(first, ROWS), pl.ds(row, cut)] if down else g_in.at[pl.ds(pl.multiple_of(first + row, cut), cut)]
        return [
            pltpu.make_async_copy(src, ring[j].at[slot], sems[family].at[slot * 4 + j])
            for j, src in enumerate((g, *(one.at[at] for one in arrays[kind])))
        ]

    def each(b, act):
        for kind in range(3):
            lo, hi = kind * BLOCKS[0], steps if kind == 2 else (kind + 1) * BLOCKS[0]
            pl.when(jnp.logical_and(b >= lo, b < hi))(lambda kind=kind, lo=lo: act(kind, b - lo))

    def start(kind, b):
        for copy in copies(kind, b, True):
            copy.start()

    def finish(kind, b):
        for copy in copies(kind, b, False):
            copy.wait()

    def step(kind, b):
        family = 1 if kind == 2 else 0
        ring = rings[family]
        slot = lax.rem(b if kind == 2 else b + kind * BLOCKS[0], DEPTH)
        for copy in copies(kind, b, True):
            copy.wait()
        g = ring[0][slot]
        g = (g.T if kind == 2 else g).astype(F32) * factor
        m = 0.9 * ring[2][slot] + 0.1 * g
        v = 0.95 * ring[3][slot] + 0.05 * g * g
        w = ring[1][slot].astype(F32)
        ring[4][slot] = (w - 0.02 * (m * lax.rsqrt(v + 1e-8) + 0.1 * w)).astype(BF)
        ring[5][slot] = m
        ring[6][slot] = v
        for copy in copies(kind, b, False):
            copy.start()

    for b in range(DEPTH):
        start(0, b)

    @pl.loop(0, steps)
    def _(b):
        pl.when(b >= DEPTH)(lambda: each(b - DEPTH, finish))
        each(b, step)
        each(b + DEPTH, start)

    pl.loop(steps - DEPTH, steps)(lambda b: each(b, finish))


def adamw(squares, summed, weights, m, v):
    any_ = pl.BlockSpec(memory_space=pl.ANY)
    dma, vmem = pltpu.SemaphoreType.DMA, pltpu.VMEM
    ring = lambda shape, turned: [vmem((DEPTH, *(turned or shape)), BF), vmem((DEPTH, *shape), BF)] + [vmem((DEPTH, *shape), F32)] * 2 + [
        vmem((DEPTH, *shape), BF)] + [vmem((DEPTH, *shape), F32)] * 2
    return pl.pallas_call(
        adamw_kernel,
        out_shape=[jax.ShapeDtypeStruct(w.shape, dtype) for dtype in (BF, F32, F32) for w in weights],
        in_specs=[pl.BlockSpec(memory_space=vmem)] + [any_] * 10,
        out_specs=[any_] * 9,
        scratch_shapes=ring((CUTS[0], COLS), None) + ring((CUTS[1], ROWS), (ROWS, CUTS[1]))
        + [dma((DEPTH * 4,)), dma((DEPTH * 4,)), dma((DEPTH * 3,)), dma((DEPTH * 3,))],
        compiler_params=pltpu.CompilerParams(vmem_limit_bytes=60 * 2**20),
        name="adamw",
    )(squares, summed, *(one for group in zip(weights, m, v, strict=True) for one in group))


MESH = pl.DeviceIdType.MESH
MATS = 6
HALF, QUARTER = ROWS // 2, ROWS // 4
N = MATS * TILES
PIECES = 2 * N
SKEW = 3
LEAD = 2
RING = 16
LINE = 4
SLOTS = 8
PART = 256


def place(q):
    return lax.rem(lax.rem(q, 3) + 2, 3) * 2 + 1 - q // 3


def backward_kernel(*refs):
    dy_in, dyt_in, a0_in, p0_in, h1_in, a1t_in, p1_in, bg_in, bu_in, wg_in, wu_in, wd_in = refs[:12]
    out, squares_out, t, p, done, arrived, swapped, right, rows_g, rows_u, bg, bu, lhs0, lhs1, by_h, small, wg, wu, wd, acc, tile, sq = refs[12:34]
    load, right_sem, xs, xr, sent, got, swap_got, back_sent, d_s, d_r, out_s, sq_s, sq_r = refs[34:]
    dp = lax.axis_index("dp")
    z, c = dp // 2, lax.rem(dp, 2)
    other = z * 2 + 1 - c
    outer = jnp.logical_or(z == 0, z == LINE - 1)
    partner = lax.select(z < LINE // 2, 1 - z, 5 - z) * 2 + c
    across = (LINE - 1 - z) * 2 + c

    def fetch(src, dst, n):
        return pltpu.make_async_copy(src, dst, load.at[n])

    get_dyt, get_a1t, get_dy, get_h1, get_wd0 = fetch(dyt_in, lhs0, 0), fetch(a1t_in, lhs1, 1), fetch(dy_in, by_h, 2), fetch(h1_in, small, 3), fetch(wd_in.at[0], wd, 4)
    get_wg1, get_wu1 = fetch(wg_in.at[1], wg, 5), fetch(wu_in.at[1], wu, 6)
    get_a0, get_wg0, get_wu0 = fetch(a0_in, small, 7), fetch(wg_in.at[0], wg, 8), fetch(wu_in.at[0], wu, 9)

    def get_rows(i):
        at = pl.ds(pl.multiple_of(i * PART, PART), PART)
        return fetch(bg_in.at[at], rows_g, 10), fetch(bu_in.at[at], rows_u, 11)

    def get_right(k):
        at = pl.ds(pl.multiple_of(lax.rem(k, TILES) * TILE, TILE), TILE)
        slot = lax.rem(k, 2)
        return [pltpu.make_async_copy(src.at[:, at], right.at[slot], right_sem.at[slot]) for src in (p1_in, bg_in, bu_in, p0_in)]

    def start_right(k):
        for q, copy in enumerate(get_right(k)):
            pl.when(k // TILES == q)(copy.start)

    get_dyt.start()
    for k in range(2):
        start_right(jnp.int32(k))
    for copy in (get_a1t, get_dy, get_h1, get_wg1, get_wu1, get_wd0, *get_rows(0)):
        copy.start()
    barrier = pltpu.get_barrier_semaphore()
    for step in range(1, 8):
        pl.semaphore_signal(barrier, inc=1, device_id={"dp": lax.rem(dp + step, 8)}, device_id_type=MESH)
    pl.semaphore_wait(barrier, 7)
    acc[...] = jnp.zeros_like(acc)

    def exchange(k):
        return pltpu.make_async_remote_copy(
            src_ref=t.at[lax.rem(k, SLOTS), pl.ds(pl.multiple_of((1 - c) * HALF, 16), HALF)],
            dst_ref=p.at[k],
            send_sem=xs.at[k],
            recv_sem=xr.at[k],
            device_id={"dp": other},
            device_id_type=MESH,
        )

    def gradient(k):
        q, slot = k // TILES, lax.rem(k, SLOTS)

        @pl.when(k >= SLOTS)
        def _():
            exchange(k - SLOTS).wait_send()

        @pl.when(q < 4)
        def _():
            get_right(k)[0].wait()

        at = pl.ds(pl.multiple_of(lax.rem(k, TILES) * TILE, TILE), TILE)
        for which, left, operand in (
            (jnp.logical_or(q == 0, q == 3), lhs0, lambda: right[lax.rem(k, 2)]),
            (jnp.logical_or(q == 1, q == 2), lhs1, lambda: right[lax.rem(k, 2)]),
            (q == 4, lhs1, lambda: bg[:, at]),
            (q == 5, lhs1, lambda: bu[:, at]),
        ):
            @pl.when(which)
            def _(left=left, operand=operand):
                t[slot] = dot(left[...], operand()).astype(BF)

        exchange(k).start()
        pl.when(k + 2 < 4 * TILES)(lambda: start_right(k + 2))

    get_dyt.wait()
    for k in range(LEAD):
        gradient(jnp.int32(k))

    def through_layer(i):
        at = pl.ds(pl.multiple_of(i * PART, PART), PART)
        for copy in get_rows(i):
            copy.wait()
        by_a = dot_t(rows_g[...], wg[...]).astype(BF) + dot_t(rows_u[...], wu[...]).astype(BF)

        @pl.when(i + 1 < TOKENS // PART)
        def _():
            for copy in get_rows(i + 1):
                copy.start()

        by_a, wide_h = by_a.astype(F32), small[at, :].astype(F32)
        scale = lax.rsqrt(jnp.mean(wide_h * wide_h, -1, keepdims=True) + 1e-6)
        inner = jnp.mean(by_a * wide_h, -1, keepdims=True)
        by_h[at, :] = by_h[at, :] + (by_a * scale - wide_h * (scale * scale * scale * inner)).astype(BF)

    def first_layer(i):
        rows = pl.ds(pl.multiple_of(i // TILES * BLOCK, BLOCK), BLOCK)
        at = pl.ds(pl.multiple_of(lax.rem(i, TILES) * TILE, TILE), TILE)
        gate, up = dot(small[rows, :], wg[:, at]), dot(small[rows, :], wu[:, at])
        bg[rows, at], bu[rows, at], _ = by_gate_and_up(gate, up, dot_t(by_h[rows, :], wd[at, :]))

    parts, firsts = TOKENS // PART, TOKENS // BLOCK * TILES
    THROUGH = 2
    TURN = THROUGH + parts
    FIRST = 2 * TURN + 2
    AGAIN = 2 * (3 * TILES - LEAD)

    def work(i):
        turn, even = i // 2, lax.rem(i, 2) == 0

        @pl.when(i == 2 * THROUGH)
        def _():
            for copy in (get_wg1, get_wu1, get_h1, get_dy, get_a1t):
                copy.wait()

        @pl.when(jnp.logical_and(even, jnp.logical_and(turn >= THROUGH, turn < TURN)))
        def _():
            through_layer(turn - THROUGH)

        @pl.when(i == 2 * TURN - 1)
        def _():
            for copy in (get_a0, get_wg0, get_wu0):
                copy.start()

        @pl.when(jnp.logical_and(even, jnp.logical_and(turn >= TURN, turn < TURN + parts)))
        def _():
            at = pl.ds(pl.multiple_of((turn - TURN) * PART, PART), PART)
            lhs0[:, at] = by_h[at, :].T

        @pl.when(i == FIRST)
        def _():
            for copy in (get_a0, get_wg0, get_wu0, get_wd0):
                copy.wait()

        @pl.when(jnp.logical_and(i >= FIRST, i < FIRST + firsts))
        def _():
            first_layer(i - FIRST)

        pl.when(jnp.logical_and(jnp.logical_not(even), turn + LEAD < N))(lambda: gradient(turn + LEAD))

        @pl.when(jnp.logical_and(i >= AGAIN, i < AGAIN + parts))
        def _():
            at = pl.ds(pl.multiple_of((i - AGAIN) * PART, PART), PART)
            lhs1[:, at] = small[at, :].T

    def wide(h, core):
        k = h // 2
        rows = pl.ds(pl.multiple_of(place(k // TILES) * ROWS + core * HALF + lax.rem(h, 2) * QUARTER, 16), QUARTER)
        return rows, pl.ds(pl.multiple_of(lax.rem(k, TILES) * TILE, TILE), TILE)

    def narrow(h):
        return h // 2, pl.ds(pl.multiple_of(lax.rem(h, 2) * QUARTER, 16), QUARTER)

    def remote(src, dst, send_sem, recv_sem, to):
        return pltpu.make_async_remote_copy(
            src_ref=src, dst_ref=dst, send_sem=send_sem, recv_sem=recv_sem, device_id={"dp": to}, device_id_type=MESH
        )

    def inward(h):
        return remote(p.at[narrow(h)], arrived.at[lax.rem(h, RING)], sent, got.at[h], partner)

    def swap(h):
        return remote(p.at[narrow(h)], swapped.at[lax.rem(h, RING)], sent, swap_got.at[h], across)

    def outward(h):
        return remote(done.at[narrow(h)], out.at[wide(h, c)], back_sent, got.at[h], partner)

    def share(h, first):
        return remote(done.at[narrow(h)] if first else out.at[wide(h, c)], out.at[wide(h, c)], d_s, d_r, other)

    def mine(h):
        k = h // 2
        pl.when(lax.rem(h, 2) == 0)(lambda: exchange(k).wait_recv())
        own = t[lax.rem(k, SLOTS), pl.ds(pl.multiple_of(c * HALF + lax.rem(h, 2) * QUARTER, 16), QUARTER)]
        return own.astype(F32) + p[narrow(h)].astype(F32)

    def valid(h):
        return jnp.logical_and(h >= 0, h < PIECES)

    def send_in(h):
        p[narrow(h)] = mine(h).astype(BF)
        inward(h).start()

    def add_and_swap(h):
        total = mine(h)
        inward(h).wait_recv()
        p[narrow(h)] = (total + arrived[lax.rem(h, RING)].astype(F32)).astype(BF)
        swap(h).start()

    def finish(h):
        swap(h).wait_recv()
        g = (p[narrow(h)].astype(F32) + swapped[lax.rem(h, RING)].astype(F32)).astype(BF)
        done[narrow(h)] = g
        outward(h).start()
        share(h, True).start()
        pltpu.make_async_copy(done.at[narrow(h)], out.at[wide(h, c)], out_s).start()
        g = g.astype(F32)
        acc[...] += jnp.sum((g * g).reshape(QUARTER // 8, 8, TILE), axis=0)

    def take(h):
        outward(h).wait_recv()
        share(h, False).start()

    @pl.loop(0, PIECES + 3 * SKEW)
    def _(i):
        @pl.when(outer)
        def _():
            pl.when(valid(i - 3 * SKEW))(lambda: take(i - 3 * SKEW))
            pl.when(valid(i))(lambda: send_in(i))

        @pl.when(jnp.logical_not(outer))
        def _():
            pl.when(valid(i - 2 * SKEW))(lambda: finish(i - 2 * SKEW))
            pl.when(valid(i - SKEW))(lambda: add_and_swap(i - SKEW))

        work(i)

    total = jnp.sum(acc[...])
    tile[...] = jnp.full(tile.shape, total, jnp.float32)

    def tell(slot, step):
        return pltpu.make_async_remote_copy(
            src_ref=tile, dst_ref=sq.at[slot], send_sem=sq_s.at[step - 1], recv_sem=sq_r.at[slot],
            device_id={"dp": lax.rem(dp + step, 8)}, device_id_type=MESH,
        )

    for slot, owner in enumerate((2, 3)):
        @pl.when(dp == owner)
        def _(slot=slot):
            for step in range(1, 8):
                tell(slot, step).start()
            sq[slot] = tile[...]

        @pl.when(dp != owner)
        def _(slot=slot):
            tell(slot, 1).wait_recv()

    squares_out[...] = sq[0] + sq[1]

    for slot, owner in enumerate((2, 3)):
        @pl.when(dp == owner)
        def _(slot=slot):
            for step in range(1, 8):
                tell(slot, step).wait_send()

    remote(p, p, sent, got.at[0], other).wait_send()
    remote(p, p, d_s, d_r, other).wait()
    pl.loop(N - SLOTS, N)(lambda k: exchange(k).wait_send())

    @pl.when(jnp.logical_not(outer))
    def _():
        remote(p, p, back_sent, got.at[0], other).wait_send()
        pltpu.make_async_copy(done, p, out_s).wait()


def backward(arrays):
    dma = pltpu.SemaphoreType.DMA
    vmem = pltpu.VMEM
    return pl.pallas_call(
        backward_kernel,
        out_shape=(jax.ShapeDtypeStruct((MATS * ROWS, COLS), BF), jax.ShapeDtypeStruct((8, 128), F32)),
        in_specs=[pl.BlockSpec(memory_space=pl.ANY)] * len(arrays),
        out_specs=(pl.BlockSpec(memory_space=pl.ANY), pl.BlockSpec(memory_space=pltpu.VMEM)),
        scratch_shapes=[
            vmem((SLOTS, ROWS, TILE), BF),
            vmem((N, HALF, TILE), BF),
            vmem((N, HALF, TILE), BF),
            vmem((RING, QUARTER, TILE), BF),
            vmem((RING, QUARTER, TILE), BF),
            vmem((2, TOKENS, TILE), BF),
            vmem((PART, COLS), BF),
            vmem((PART, COLS), BF),
            vmem((TOKENS, COLS), BF),
            vmem((TOKENS, COLS), BF),
            vmem((ROWS, TOKENS), BF),
            vmem((ROWS, TOKENS), BF),
            vmem((TOKENS, ROWS), BF),
            vmem((TOKENS, ROWS), BF),
            vmem((ROWS, COLS), BF),
            vmem((ROWS, COLS), BF),
            vmem((COLS, ROWS), BF),
            vmem((8, TILE), F32),
            vmem((8, 128), F32),
            vmem((2, 8, 128), F32),
            dma((12,)), dma((2,)), dma((N,)), dma((N,)), dma(()), dma((PIECES,)), dma((PIECES,)), dma(()), dma(()), dma(()), dma(()),
            dma((7,)), dma((2,)),
        ],
        compiler_params=pltpu.CompilerParams(collective_id=0, has_side_effects=True, vmem_limit_bytes=67043328),
        name="backward",
    )(*arrays)


def solution(mesh):
    def step(x, dy, *arrays):
        weights, m, v = (arrays[i : i + 3] for i in (0, 3, 6))
        x, dy = x[0], dy[0]
        kept = forward(x, dy, *weights)
        summed, squares = backward((dy, *kept, *weights))
        return tuple(adamw(squares, summed, weights, m, v))

    return jax.shard_map(
        step,
        mesh=mesh,
        in_specs=(P(("rep", "dp"), None, None),) * 2 + (P(None, None, None),) * 9,
        out_specs=(P("rep", None, None),) * 9,
        check_vma=False,
    )
```
